128 devices in a mesh: px: 8 (over y_hi, z), py: 16 (over y_lo, x, core).
Axes of the slice: x: 4, y: 4 (y_hi: 2, y_lo: 2; y = y_hi * 2 + y_lo), z: 4, core: 2. Of those that a mesh axis runs over, the one named last changes fastest.
Arguments:
- vorticity: float32 [3, 192, 36864], P(None, 'px', 'py'), may hold values from -6 to 6
Outputs:
- velocity: float32 [3, 192, 36864], P(None, 'px', 'py')
- stretching: float32 [3, 192, 36864], P(None, 'px', 'py')
The draws below stay inside these ranges and needn't reach their ends.
All inputs are finite; a program needn't handle non-finite values.
Results may differ from the reference program's by a relative error of at most 0.0003.
Values sent between devices are 32-bit elements; how exact they have to be, the bound alone decides.
A program may use at most 128 MiB of HBM per device.

```python
import math
import jax
import jax.numpy as jnp
from jax import lax

G = 192


def draw_vorticity(key, part):
    noise_key = jax.random.fold_in(key, 11)
    values = jax.random.normal(noise_key, (3, G, G, G), jnp.float32)
    return jnp.clip(values, -6.0, 6.0).reshape(3, G, G * G)


def setup_inputs(seed: int = 0) -> dict:
    streams_of = jax.random.split(jax.random.key(seed), 2)
    vorticity = draw_vorticity(jax.random.fold_in(streams_of[1], 71), 0)
    return {"vorticity": vorticity}


smoothing = 1.0


def window(padded, axis, offset):
    starts = [0, 2, 2, 2]
    limits = [padded.shape[0], padded.shape[1] - 2, padded.shape[2] - 2, padded.shape[3] - 2]
    starts[axis] = starts[axis] + offset
    limits[axis] = limits[axis] + offset
    return lax.slice(padded, starts, limits)


def derivative(padded, axis):
    near = window(padded, axis, 1) - window(padded, axis, -1)
    far = window(padded, axis, 2) - window(padded, axis, -2)
    return (8.0 * near - far) / 12.0


def reference(vorticity):
    field = vorticity.reshape(3, G, G, G)
    length = 2 * G
    index = jnp.arange(length, dtype=jnp.int32)
    signed = jnp.where(index < length // 2, index, index - length)
    wave = signed.astype(jnp.float32) * (2.0 * math.pi / length)
    slope = jnp.where(index == length // 2, 0.0, wave)
    keep = jnp.where(index == length // 2, 0.0, 1.0)
    half_index = jnp.arange(length // 2 + 1, dtype=jnp.int32)
    half_wave = half_index.astype(jnp.float32) * (2.0 * math.pi / length)
    half_slope = jnp.where(half_index == length // 2, 0.0, half_wave)
    half_keep = jnp.where(half_index == length // 2, 0.0, 1.0)
    square = wave[:, None, None] ** 2 + wave[None, :, None] ** 2 + half_wave[None, None, :] ** 2
    mask = keep[:, None, None] * keep[None, :, None] * half_keep[None, None, :]
    green = mask * jnp.exp(-0.5 * smoothing * smoothing * square) / (square + jnp.where(square == 0.0, 1.0, 0.0))
    slope_x = slope[:, None, None]
    slope_y = slope[None, :, None]
    slope_z = half_slope[None, None, :]
    potential = []
    for component in range(3):
        spread = jnp.pad(field[component], ((0, G), (0, G), (0, G)))
        potential.append(jnp.fft.rfftn(spread) * green)
    terms = [slope_y * potential[2] - slope_z * potential[1],
             slope_z * potential[0] - slope_x * potential[2],
             slope_x * potential[1] - slope_y * potential[0]]
    fields = []
    for component in range(3):
        back = jnp.fft.irfftn(1j * terms[component], s=(length, length, length))
        fields.append(back[:G, :G, :G].astype(jnp.float32))
    flow = jnp.stack(fields)
    padded = jnp.pad(flow, ((0, 0), (2, 2), (2, 2), (2, 2)))
    stretching = (field[0] * derivative(padded, 1) + field[1] * derivative(padded, 2)
                  + field[2] * derivative(padded, 3))
    return flow.reshape(3, G, G * G), stretching.reshape(3, G, G * G)
```

```python
import math
import functools

import numpy as np
import jax
import jax.numpy as jnp
from jax import lax
from jax.experimental import pallas as pl
from jax.experimental.pallas import tpu as pltpu
from jax.sharding import PartitionSpec as P

G = 192
N = 2 * G
MESH = pl.DeviceIdType.MESH
VMEM = pltpu.VMEM
ANY = pl.ANY
bf16 = jnp.bfloat16
f32 = jnp.float32


def split_np(t):
    hi = np.asarray(t, np.float32).astype(jnp.bfloat16)
    lo = (t - hi.astype(np.float64)).astype(np.float32).astype(jnp.bfloat16)
    return hi, lo


def wide_lhs(t):
    hi, lo = split_np(t)
    return np.concatenate([hi, hi, lo], axis=-1)


def tall_rhs(t):
    hi, lo = split_np(t)
    return np.concatenate([hi, hi, lo], axis=-2)


def trig(m, t, j):
    a = 2.0 * np.pi * ((m * j) % N) / N
    return np.where(t == 0, np.cos(a), np.sin(a))


def tables():
    w = lambda m: np.where(m == 0, 1.0, 2.0) / N
    r = np.arange(384)
    dg, zm, dl = r // 48, (r // 8) % 6, r % 8
    mz, tz = 3 * (8 * dg + dl) + zm // 2, zm % 2
    z = np.arange(256)
    zf = np.where(z[None] < G, trig(mz[:, None], tz[:, None], z[None]), 0.0)
    zi = (zf * w(mz)[:, None]).T
    my, ty = 2 * (r % 96) + r // 192, (r // 96) % 2
    k = np.arange(192)
    jy = 12 * (k % 16) + k // 16
    yf = trig(my[:, None], ty[:, None], jy[None])
    yi = (yf * w(my)[:, None]).T
    yi2 = np.stack([yi, np.concatenate([yi[:, 192:], yi[:, :192]], 1)])
    mx, tx = 64 * (r // 128) + r % 64, (r // 64) % 2
    lane = np.arange(128)
    xf = []
    for c in range(2):
        rows = []
        for side in (c, 1 - c):
            j = 96 * side + lane
            rows.append(np.where(lane[:, None] < 96, trig(mx[None], tx[None], j[:, None]), 0.0))
        xf.append(np.concatenate(rows, 0))
    xf = np.stack(xf)
    xi = np.swapaxes(xf * w(mx)[None, None], 1, 2)
    return dict(
        zf=wide_lhs(zf), zi=wide_lhs(zi), yf=wide_lhs(yf), yi=wide_lhs(yi2),
        xf=tall_rhs(xf), xi=tall_rhs(xi),
    )


def split(x):
    hi = x.astype(bf16)
    lo = (x - hi.astype(f32)).astype(bf16)
    return hi, lo


def lanes(shape):
    return lax.broadcasted_iota(jnp.int32, shape, len(shape) - 1)


def dot(a, b, rhs_t=False):
    return lax.dot_general(a, b, (((1,), (1 if rhs_t else 0,)), ((), ())), preferred_element_type=f32)


def z_forward_kernel(vort, tz, out, w):
    lane = lanes((24, 128))
    zero = jnp.zeros((24, 128), f32)
    for y in range(12):
        for c in range(3):
            a, b, d = [vort[c, :, pl.ds(384 * (y // 2) + 128 * i, 128)] for i in range(3)]
            if y % 2 == 0:
                v0, v1 = a, jnp.where(lane < 64, b, zero)
            else:
                rb, rd = pltpu.roll(b, 64, 1), pltpu.roll(d, 64, 1)
                v0, v1 = jnp.where(lane < 64, rb, rd), jnp.where(lane < 64, rd, zero)
            r0 = y * 72 + c * 24
            w[pl.ds(r0, 24), pl.ds(0, 128)] = v0
            w[pl.ds(r0, 24), pl.ds(128, 128)] = v1
    w[pl.ds(864, 32), :] = jnp.zeros((32, 256), f32)
    for blk, n in ((0, 256), (256, 256), (512, 256), (768, 128)):
        hi, lo = split(w[pl.ds(blk, n), :])
        acc = dot(tz[...], jnp.concatenate([hi, lo, hi], axis=1), rhs_t=True)
        for jj in range(n // 128):
            out[:, :, blk // 128 + jj] = acc[:, 128 * jj : 128 * jj + 128].reshape(8, 6, 8, 128)


def vcall(kernel, out, n_in, **kw):
    single = not isinstance(out, (tuple, list))
    params = dict(vmem_limit_bytes=60 * 1024 * 1024)
    params.update(kw.pop("params", {}))
    return pl.pallas_call(
        kernel,
        out_shape=out,
        in_specs=[pl.BlockSpec(memory_space=VMEM)] * n_in,
        out_specs=pl.BlockSpec(memory_space=VMEM) if single else [pl.BlockSpec(memory_space=VMEM)] * len(out),
        compiler_params=pltpu.CompilerParams(**params),
        **kw,
    )


def sds(*shape):
    return jax.ShapeDtypeStruct(shape, f32)


def forward_exchange_kernel(src, dst, ssem, rsem):
    p, q = lax.axis_index("px"), lax.axis_index("py")
    bar = pltpu.get_barrier_semaphore()

    def greet(i, _):
        pl.semaphore_signal(bar, inc=1, device_id=((q % 2) * 4 + i // 16, i % 16), device_id_type=MESH)
        return 0

    lax.fori_loop(0, 64, greet, 0)
    pl.semaphore_wait(bar, 64)
    slot = (p % 4) * 16 + q

    def send(i, _):
        a, b = (p + i // 8) % 8, (q // 2 + i) % 8
        qd = 2 * b + p // 4
        s = src.at[a, :, :, b]
        t = dst.at[:, p % 4, q // 8, :, q % 8]
        me = jnp.logical_and(a == p, qd == q)

        @pl.when(me)
        def _():
            pltpu.make_async_copy(s, t, rsem.at[slot]).start()

        @pl.when(jnp.logical_not(me))
        def _():
            pltpu.make_async_remote_copy(s, t, ssem.at[i], rsem.at[slot], device_id=(a, qd), device_id_type=MESH).start()

        return 0

    lax.fori_loop(0, 64, send, 0)

    def wait(i, _):
        a, b = (p + i // 8) % 8, (q // 2 + i) % 8
        s = src.at[a, :, :, b]
        me = jnp.logical_and(a == p, 2 * b + p // 4 == q)

        @pl.when(jnp.logical_not(me))
        def _():
            pltpu.make_async_copy(s, s, ssem.at[i]).wait()

        t = dst.at[:, i // 16, (i % 16) // 8, :, i % 8]
        pltpu.make_async_copy(t, t, rsem.at[i]).wait()
        return 0

    lax.fori_loop(0, 64, wait, 0)


def backward_exchange_kernel(src, dst, ssem, rsem):
    p, q = lax.axis_index("px"), lax.axis_index("py")
    bar = pltpu.get_barrier_semaphore()

    def greet(i, _):
        pl.semaphore_signal(bar, inc=1, device_id=(i // 8, 2 * (i % 8) + p // 4), device_id_type=MESH)
        return 0

    lax.fori_loop(0, 64, greet, 0)
    pl.semaphore_wait(bar, 64)
    slot = p * 8 + q // 2

    def send(i, _):
        al, b = (p + i // 16) % 4, (q + i) % 16
        a = (q % 2) * 4 + al
        s = src.at[:, al, b // 8, :, b % 8]
        t = dst.at[p, :, :, q // 2]
        me = jnp.logical_and(a == p, b == q)

        @pl.when(me)
        def _():
            pltpu.make_async_copy(s, t, rsem.at[slot]).start()

        @pl.when(jnp.logical_not(me))
        def _():
            pltpu.make_async_remote_copy(s, t, ssem.at[i], rsem.at[slot], device_id=(a, b), device_id_type=MESH).start()

        return 0

    lax.fori_loop(0, 64, send, 0)

    def wait(i, _):
        al, b = (p + i // 16) % 4, (q + i) % 16
        s = src.at[:, al, b // 8, :, b % 8]
        me = jnp.logical_and((q % 2) * 4 + al == p, b == q)

        @pl.when(jnp.logical_not(me))
        def _():
            pltpu.make_async_copy(s, s, ssem.at[i]).wait()

        t = dst.at[i // 8, :, :, i % 8]
        pltpu.make_async_copy(t, t, rsem.at[i]).wait()
        return 0

    lax.fori_loop(0, 64, wait, 0)


def exchange(kernel, x, out, cid):
    return pl.pallas_call(
        kernel,
        out_shape=out,
        in_specs=[pl.BlockSpec(memory_space=VMEM)],
        out_specs=pl.BlockSpec(memory_space=VMEM),
        scratch_shapes=[pltpu.SemaphoreType.DMA((64,)), pltpu.SemaphoreType.DMA((64,))],
        compiler_params=pltpu.CompilerParams(collective_id=cid, has_side_effects=True),
    )(x)


def partner_kernel(pick, src, dst, ssem, rsem):
    p, q = lax.axis_index("px"), lax.axis_index("py")
    other = q + 1 - 2 * (q % 2)
    bar = pltpu.get_barrier_semaphore()
    pl.semaphore_signal(bar, inc=1, device_id=(p, other), device_id_type=MESH)
    pl.semaphore_wait(bar, 1)
    s = src.at[1 - q % 2] if pick else src
    cp = pltpu.make_async_remote_copy(s, dst, ssem, rsem, device_id=(p, other), device_id_type=MESH)
    cp.start()
    cp.wait()


def to_partner(x, pick, cid):
    return pl.pallas_call(
        functools.partial(partner_kernel, pick),
        out_shape=sds(18, 192, 128),
        in_specs=[pl.BlockSpec(memory_space=VMEM)],
        out_specs=pl.BlockSpec(memory_space=VMEM),
        scratch_shapes=[pltpu.SemaphoreType.DMA, pltpu.SemaphoreType.DMA],
        compiler_params=pltpu.CompilerParams(collective_id=cid, has_side_effects=True),
    )(x)


def y_forward_kernel(r, ty, out, s):
    lane = lanes((8, 128))
    zero = jnp.zeros((8, 128), f32)

    def body(zm, _):
        for y in range(12):
            for c in range(3):
                j, o = divmod(24 * (3 * y + c), 128)
                for qh in range(2):
                    v = zero
                    for pp in (3, 2, 1, 0):
                        t = r[zm, pp, qh, j]
                        if o + 24 > 128:
                            t = jnp.where(lane >= o, t, r[zm, pp, qh, j + 1])
                        t = pltpu.roll(t, (24 * pp - o) % 128, 1)
                        v = jnp.where(lane < 24 * pp + 24, t, v)
                    s[pl.ds(8 * (2 * y + qh), 8), pl.ds(128 * c, 128)] = v
        hi, lo = split(s[...])
        acc = dot(ty[...], jnp.concatenate([hi, lo, hi], axis=0))
        for h in range(2):
            for c in range(3):
                out[h, 3 * zm + c] = acc[192 * h : 192 * h + 192, 128 * c : 128 * c + 128]
        return 0

    lax.fori_loop(0, 6, body, 0)


def x_kernel(mine, theirs, xf, xi, um, uo, f, u):
    p, q = lax.axis_index("px"), lax.axis_index("py")
    core = q % 2
    chip = p * 8 + q // 2
    unit = 2.0 * math.pi / N
    lane = lanes((8, 128))
    row = lax.broadcasted_iota(jnp.int32, (8, 128), 0)
    sign = jnp.where(lane % 128 < 64, 1.0, -1.0)
    B = 48

    def body(it, _):
        g, ib = it // 2, it % 2
        kz = (3 * chip + g).astype(f32) * unit
        parts = []
        for t in range(2):
            for c in range(3):
                zmc = (2 * g + t) * 3 + c
                for s in range(2):
                    rows = pl.ds(pl.multiple_of(96 * s + B * ib, 8), B)
                    parts.append(jnp.concatenate([mine[core, zmc, rows, :], theirs[zmc, rows, :]], axis=1))
        hi, lo = split(jnp.concatenate(parts, axis=0))
        f[...] = dot(jnp.concatenate([hi, lo, hi], axis=1), xf[core])

        def mix(rt, _):
            ky = ((2 * (B * ib + 8 * rt) + core) + 2 * row).astype(f32) * unit
            for tl in range(3):
                kx = (64 * tl + lane % 64).astype(f32) * unit
                sq = kx * kx + ky * ky + kz * kz
                green = jnp.exp(-0.5 * sq) / (sq + jnp.where(sq == 0.0, 1.0, 0.0))
                kxs = kx * sign
                ls = pl.ds(128 * tl, 128)
                rs = lambda t, c, s: pl.ds(pl.multiple_of(((t * 3 + c) * 2 + s) * B + 8 * rt, 8), 8)
                pt = [[[f[rs(t, c, s), ls] * green for s in range(2)] for c in range(3)] for t in range(2)]
                for t in range(2):
                    dz = (lambda c, s: kz * pt[1][c][s]) if t == 0 else (lambda c, s: -kz * pt[0][c][s])
                    for s in range(2):
                        dy = (lambda c: ky * pt[t][c][1]) if s == 0 else (lambda c: -ky * pt[t][c][0])
                        dx = lambda c: kxs * pltpu.roll(pt[t][c][s], 64, 1)
                        u[rs(t, 0, s), ls] = dy(2) - dz(1, s)
                        u[rs(t, 1, s), ls] = dz(0, s) - dx(2)
                        u[rs(t, 2, s), ls] = dx(1) - dy(0)
            return 0

        lax.fori_loop(0, B // 8, mix, 0)
        hi, lo = split(u[...])
        back = dot(jnp.concatenate([hi, lo, hi], axis=1), xi[core])
        for t in range(2):
            for c in range(3):
                for s in range(2):
                    zmc = (2 * g + t) * 3 + c
                    rows = pl.ds(pl.multiple_of(96 * s + B * ib, 8), B)
                    r0 = ((t * 3 + c) * 2 + s) * B
                    um[zmc, rows, :] = back[r0 : r0 + B, :128]
                    uo[zmc, rows, :] = back[r0 : r0 + B, 128:]
        return 0

    lax.fori_loop(0, 6, body, 0)


def y_backward_kernel(um, ru, ty, out, o):
    core = lax.axis_index("py") % 2
    lane = lanes((8, 128))

    def body(zm, _):
        top = jnp.concatenate([um[3 * zm + c] for c in range(3)], axis=1)
        low = jnp.concatenate([ru[3 * zm + c] for c in range(3)], axis=1)
        hi, lo = split(jnp.concatenate([top, low], axis=0))
        o[...] = dot(ty[core], jnp.concatenate([hi, lo, hi], axis=0))
        for pp in range(4):
            for qh in range(2):
                for j in range(7):
                    v = None
                    for g in range((128 * j) // 24, min((128 * j + 127) // 24, 35) + 1):
                        y, c = divmod(g, 3)
                        t = o[pl.ds(8 * (2 * y + qh), 8), pl.ds(128 * c, 128)]
                        t = pltpu.roll(t, (24 * g - 128 * j - 24 * pp) % 128, 1)
                        v = t if v is None else jnp.where(lane >= 24 * g - 128 * j, t, v)
                    out[zm, pp, qh, j] = v
        return 0

    lax.fori_loop(0, 6, body, 0)


def z_backward_kernel(v, tz, flow, vel, s):
    for j in range(7):
        hi, lo = split(v[:, :, j].reshape(384, 128))
        acc = dot(tz[...], jnp.concatenate([hi, lo, hi], axis=0))
        s[pl.ds(128 * j, 128), :] = acc.T
    lane = lanes((24, 128))
    for c in range(3):
        for yp in range(6):
            t = []
            for e in range(2):
                y = 2 * yp + e
                r0 = y * 72 + c * 24
                a, b = s[pl.ds(r0, 24), pl.ds(0, 128)], s[pl.ds(r0, 24), pl.ds(128, 128)]
                flow[3 * y + c, :, pl.ds(0, 128)] = a
                flow[3 * y + c, :, pl.ds(128, 128)] = b
                t.append((a, b))
            (a0, b0), (a1, b1) = t
            ra, rb = pltpu.roll(a1, 64, 1), pltpu.roll(b1, 64, 1)
            vel[c, :, pl.ds(384 * yp, 128)] = a0
            vel[c, :, pl.ds(384 * yp + 128, 128)] = jnp.where(lane < 64, b0, ra)
            vel[c, :, pl.ds(384 * yp + 256, 128)] = jnp.where(lane < 64, ra, rb)


def stretch_kernel(flow, w, st, pad, xs, xr, yr, sems):
    p, q = lax.axis_index("px"), lax.axis_index("py")
    has_l, has_r, has_d, has_u = p > 0, p < 7, q > 0, q < 15
    near = [(has_l, (p - 1, q)), (has_r, (p + 1, q)), (has_d, (p, q - 1)), (has_u, (p, q + 1))]
    bar = pltpu.get_barrier_semaphore()
    for has, dev in near:
        @pl.when(has)
        def _():
            pl.semaphore_signal(bar, inc=1, device_id=dev, device_id_type=MESH)
    count = sum(h.astype(jnp.int32) for h, _ in near)
    pl.semaphore_wait(bar, count)

    for m in range(9):
        for e, r0 in ((0, 0), (1, 22)):
            for i in range(4):
                xs[e, m, pl.ds(2 * i, 2), :] = flow[4 * m + i, pl.ds(r0, 2), :]
    cps = []
    srcs = [xs.at[0], xs.at[1], flow.at[pl.ds(0, 6)], flow.at[pl.ds(30, 6)]]
    dsts = [xr.at[1], xr.at[0], yr.at[1], yr.at[0]]
    back = [1, 0, 3, 2]
    for k, (has, dev) in enumerate(near):
        cp = pltpu.make_async_remote_copy(srcs[k], dsts[k], sems.at[0, k], sems.at[1, k], device_id=dev, device_id_type=MESH)
        cps.append(cp)

        @pl.when(has)
        def _(cp=cp):
            cp.start()

    zx, zy = jnp.zeros((9, 8, 256), f32), jnp.zeros((6, 24, 256), f32)
    for k, ref, zero in ((0, xr.at[0], zx), (1, xr.at[1], zx), (2, yr.at[0], zy), (3, yr.at[1], zy)):
        @pl.when(jnp.logical_not(near[k][0]))
        def _(ref=ref, zero=zero):
            ref[...] = zero

    for i in range(36):
        pad[i, pl.ds(8, 24), :] = flow[i]
    for k, (has, dev) in enumerate(near):
        @pl.when(has)
        def _(k=k):
            cps[k].wait_send()
            cps[back[k]].wait_recv()
    for i in range(36):
        pad[i, pl.ds(6, 2), :] = xr[0, i // 4, pl.ds(2 * (i % 4), 2), :]
        pad[i, pl.ds(32, 2), :] = xr[1, i // 4, pl.ds(2 * (i % 4), 2), :]

    def at_y(y, c):
        if y < 0:
            return yr[0, (y + 2) * 3 + c]
        if y >= 12:
            return yr[1, (y - 12) * 3 + c]
        return flow[3 * y + c]

    def diff(m2, m1, p1, p2):
        return (8.0 * (p1 - m1) - (p2 - m2)) * (1.0 / 12.0)

    lane = lanes((24, 128))
    for c in range(3):
        for yp in range(6):
            t = []
            for y in (2 * yp, 2 * yp + 1):
                i = 3 * y + c
                wv = [w[pl.ds(72 * y + 24 * d, 24), :] for d in range(3)]
                dx = diff(*[pad[i, pl.ds(8 + o, 24), :] for o in (-2, -1, 1, 2)])
                dy = diff(*[at_y(y + o, c) for o in (-2, -1, 1, 2)])
                cur = flow[i]
                dz = diff(*[pltpu.roll(cur, (-o) % 256, 1) for o in (-2, -1, 1, 2)])
                r = wv[0] * dx + wv[1] * dy + wv[2] * dz
                t.append((r[:, :128], r[:, 128:]))
            (a0, b0), (a1, b1) = t
            ra, rb = pltpu.roll(a1, 64, 1), pltpu.roll(b1, 64, 1)
            st[c, :, pl.ds(384 * yp, 128)] = a0
            st[c, :, pl.ds(384 * yp + 128, 128)] = jnp.where(lane < 64, b0, ra)
            st[c, :, pl.ds(384 * yp + 256, 128)] = jnp.where(lane < 64, ra, rb)


def on_device(tb, vort):
    zt, w = vcall(z_forward_kernel, [sds(8, 6, 7, 8, 128), sds(896, 256)], 2)(vort, tb["zf"])
    rows = exchange(forward_exchange_kernel, zt.reshape(8, 6, 7, 8, 1, 128), sds(6, 4, 2, 7, 8, 1, 128), 0)
    yt = vcall(y_forward_kernel, sds(2, 18, 192, 128), 2, scratch_shapes=[VMEM((192, 384), f32)])(
        rows.reshape(6, 4, 2, 7, 8, 128), tb["yf"]
    )
    theirs = to_partner(yt, True, 1)
    um, uo = vcall(
        x_kernel, [sds(18, 192, 128), sds(18, 192, 128)], 4,
        scratch_shapes=[VMEM((576, 384), f32), VMEM((576, 384), f32)],
    )(yt, theirs, tb["xf"], tb["xi"])
    ru = to_partner(uo, False, 2)
    back = vcall(y_backward_kernel, sds(6, 4, 2, 7, 8, 128), 3, scratch_shapes=[VMEM((192, 384), f32)])(um, ru, tb["yi"])
    v = exchange(backward_exchange_kernel, back.reshape(6, 4, 2, 7, 8, 1, 128), sds(8, 6, 7, 8, 1, 128), 3)
    flow, vel = vcall(
        z_backward_kernel, [sds(36, 24, 256), sds(3, 24, 2304)], 2, scratch_shapes=[VMEM((896, 256), f32)]
    )(v.reshape(8, 6, 7, 8, 128), tb["zi"])
    st = vcall(
        stretch_kernel, sds(3, 24, 2304), 2,
        scratch_shapes=[
            VMEM((36, 40, 256), f32), VMEM((2, 9, 8, 256), f32), VMEM((2, 9, 8, 256), f32), VMEM((2, 6, 24, 256), f32),
            pltpu.SemaphoreType.DMA((2, 4)),
        ],
        params=dict(collective_id=4, has_side_effects=True),
    )(flow, w)
    return vel, st


def solution(mesh):
    tb = {k: jnp.asarray(v) for k, v in tables().items()}
    return jax.shard_map(
        functools.partial(on_device, tb), mesh=mesh, in_specs=(P(None, "px", "py"),),
        out_specs=(P(None, "px", "py"), P(None, "px", "py")), check_vma=False,
    )
```

```python
import math
import functools

import numpy as np
import jax
import jax.numpy as jnp
from jax import lax
from jax.experimental import pallas as pl
from jax.experimental.pallas import tpu as pltpu
from jax.sharding import PartitionSpec as P

G = 192
N = 2 * G
MESH = pl.DeviceIdType.MESH
VMEM = pltpu.VMEM
ANY = pl.ANY
bf16 = jnp.bfloat16
f32 = jnp.float32


def pair_np(t):
    hi = np.asarray(t, np.float32).astype(jnp.bfloat16)
    lo = (t - hi.astype(np.float64)).astype(np.float32).astype(jnp.bfloat16)
    return hi, lo


def trig(m, t, j):
    a = 2.0 * np.pi * ((m * j) % N) / N
    return np.where(t == 0, np.cos(a), np.sin(a))


def weight(m):
    return np.where(m == 0, 1.0, 2.0) / N


def tables():
    r = np.arange(384)
    dg, zm, dl = r // 48, (r // 8) % 6, r % 8
    mz, tz = 3 * (8 * dg + dl) + zm // 2, zm % 2
    z = np.arange(256)
    zf = np.where(z[None] < G, trig(mz[:, None], tz[:, None], z[None]), 0.0)
    zi = (zf * weight(mz)[:, None]).T.reshape(256, 8, 3, 2, 8).transpose(2, 0, 1, 3, 4).reshape(3, 256, 128)
    my, ty = 2 * (r % 96) + r // 192, (r // 96) % 2
    k = np.arange(192)
    jy = 12 * (k % 16) + k // 16
    yf = trig(my[:, None], ty[:, None], jy[None])
    yi = (yf * weight(my)[:, None]).T
    mx, tx = 64 * (r // 128) + r % 64, (r // 64) % 2
    lane = np.arange(128)
    jx = 96 * np.arange(2)[:, None] + lane[None]
    xf = np.where(lane[None, :, None] < 96, trig(mx[None, None], tx[None, None], jx[:, :, None]), 0.0)
    xi = np.swapaxes(xf * weight(mx)[None, None], 1, 2)
    stack = lambda t: np.stack(pair_np(t), axis=-3)
    wide = lambda t: np.concatenate([pair_np(t)[0], pair_np(t)[0], pair_np(t)[1]], axis=-1)
    return [stack(zf), wide(yf), stack(xf), stack(xi), wide(yi), stack(zi)]


def split(x):
    hi = x.astype(bf16)
    lo = (x - hi.astype(f32)).astype(bf16)
    return hi, lo


def cat(parts, axis):
    return jnp.concatenate(parts, axis=axis)


def lanes(shape):
    return lax.broadcasted_iota(jnp.int32, shape, len(shape) - 1)


def dot(a, b, rhs_t=False):
    return lax.dot_general(a, b, (((1,), (1 if rhs_t else 0,)), ((), ())), preferred_element_type=f32)


def padded_line(vort, c, y, lane):
    a, b, d = [vort[c, :, pl.ds(384 * (y // 2) + 128 * i, 128)] for i in range(3)]
    if y % 2 == 0:
        return a, jnp.where(lane < 64, b, 0.0)
    rb, rd = pltpu.roll(b, 64, 1), pltpu.roll(d, 64, 1)
    return jnp.where(lane < 64, rb, rd), jnp.where(lane < 64, rd, 0.0)


def z_forward(vort, zf, out, w):
    lane = lanes((24, 128))
    for y in range(12):
        for c in range(3):
            v0, v1 = padded_line(vort, c, y, lane)
            r0 = y * 72 + c * 24
            w[pl.ds(r0, 24), pl.ds(0, 128)] = v0
            w[pl.ds(r0, 24), pl.ds(128, 128)] = v1
    w[pl.ds(864, 32), :] = jnp.zeros((32, 256), f32)
    table = cat([zf[0], zf[0], zf[1]], 1)
    for blk, n in ((0, 256), (256, 256), (512, 256), (768, 128)):
        hi, lo = split(w[pl.ds(blk, n), :])
        acc = dot(table, cat([hi, lo, hi], 1), rhs_t=True)
        for jj in range(n // 128):
            out[:, :, blk // 128 + jj] = acc[:, 128 * jj : 128 * jj + 128].reshape(8, 6, 8, 128)


def y_forward(zm, r, ty, out, s):
    lane = lanes((8, 128))
    zero = jnp.zeros((8, 128), f32)
    for y in range(12):
        for c in range(3):
            j, o = divmod(24 * (3 * y + c), 128)
            for qh in range(2):
                v = zero
                for pp in (3, 2, 1, 0):
                    t = r[zm, pp, qh, j]
                    if o + 24 > 128:
                        t = jnp.where(lane >= o, t, r[zm, pp, qh, j + 1])
                    t = pltpu.roll(t, (24 * pp - o) % 128, 1)
                    v = jnp.where(lane < 24 * pp + 24, t, v)
                s[pl.ds(8 * (2 * y + qh), 8), pl.ds(128 * c, 128)] = v
    hi, lo = split(s[...])
    acc = dot(ty[...], cat([hi, lo, hi], 0))
    for h in range(2):
        for c in range(3):
            out[h, 3 * zm + c] = acc[192 * h : 192 * h + 192, 128 * c : 128 * c + 128]


def green_table(chip, core, out):
    unit = 2.0 * math.pi / N
    lane = lanes((8, 128))
    row = lax.broadcasted_iota(jnp.int32, (8, 128), 0)

    def body(it, _):
        kz = (3 * chip + it // 12).astype(f32) * unit
        ky = (16 * (it % 12) + core + 2 * row).astype(f32) * unit
        for tl in range(3):
            kx = (64 * tl + lane % 64).astype(f32) * unit
            sq = kx * kx + ky * ky + kz * kz
            green = jnp.exp(-0.5 * sq) / (sq + jnp.where(sq == 0.0, 1.0, 0.0))
            out[pl.ds(pl.multiple_of(8 * it, 8), 8), pl.ds(128 * tl, 128)] = green
        return 0

    lax.fori_loop(0, 36, body, 0)


B = 48


def x_stage(g, chip, core, yt, th, xf, xi, gt, ub, uo, f, u):
    unit = 2.0 * math.pi / N
    lane = lanes((8, 128))
    row = lax.broadcasted_iota(jnp.int32, (8, 128), 0)
    sign = jnp.where(lane < 64, 1.0, -1.0)
    kz = (3 * chip + g).astype(f32) * unit
    combos = [(t, c, s) for t in range(2) for c in range(3) for s in range(2)]
    at = lambda t, c, s: ((t * 3 + c) * 2 + s) * B
    tf = cat([xf[core, 0], xf[1 - core, 0], xf[core, 0], xf[1 - core, 0], xf[core, 1], xf[1 - core, 1]], 0)
    for ib in range(2):
        parts = []
        for t, c, s in combos:
            rows = pl.ds(96 * s + B * ib, B)
            zmc = 6 * g + 3 * t + c
            parts.append(cat([yt[core, zmc, rows, :], th[zmc, rows, :]], 1))
        hi, lo = split(cat(parts, 0))
        f[ib] = dot(cat([hi, lo, hi], 1), tf)
    for ib in range(2):
        for rt in range(B // 8):
            i0 = B * ib + 8 * rt
            ky = (2 * i0 + core + 2 * row).astype(f32) * unit
            for tl in range(3):
                kxs = (64 * tl + lane % 64).astype(f32) * unit * sign
                ls = pl.ds(128 * tl, 128)
                green = gt[pl.ds(pl.multiple_of(96 * g + i0, 8), 8), ls]
                pt = {k: f[ib, pl.ds(at(*k) + 8 * rt, 8), ls] * green for k in combos}
                for t in range(2):
                    dz = lambda c, s: (kz if t == 0 else -kz) * pt[1 - t, c, s]
                    for s in range(2):
                        dy = lambda c: (ky if s == 0 else -ky) * pt[t, c, 1 - s]
                        dx = lambda c: kxs * pltpu.roll(pt[t, c, s], 64, 1)
                        u[ib, pl.ds(at(t, 0, s) + 8 * rt, 8), ls] = dy(2) - dz(1, s)
                        u[ib, pl.ds(at(t, 1, s) + 8 * rt, 8), ls] = dz(0, s) - dx(2)
                        u[ib, pl.ds(at(t, 2, s) + 8 * rt, 8), ls] = dx(1) - dy(0)
    k0 = cat([xi[core, 0], xi[1 - core, 0]], 1)
    k1 = cat([xi[core, 1], xi[1 - core, 1]], 1)
    ti = cat([k0, k0, k1], 0)
    for ib in range(2):
        hi, lo = split(u[ib])
        back = dot(cat([hi, lo, hi], 1), ti)
        for t, c, s in combos:
            rows = pl.ds(96 * s + B * ib, B)
            zmc = 6 * g + 3 * t + c
            r0 = at(t, c, s)
            ub[core, zmc, rows, :] = back[r0 : r0 + B, :128]
            uo[zmc, rows, :] = back[r0 : r0 + B, 128:]


def y_backward(zm, ub, ty, out, o):
    lane = lanes((8, 128))
    rhs = cat([cat([ub[h, 3 * zm + c] for c in range(3)], 1) for h in range(2)], 0)
    hi, lo = split(rhs)
    o[...] = dot(ty[...], cat([hi, lo, hi], 0))
    for pp in range(4):
        for qh in range(2):
            for j in range(7):
                v = None
                for g in range((128 * j) // 24, min((128 * j + 127) // 24, 35) + 1):
                    y, c = divmod(g, 3)
                    t = o[pl.ds(8 * (2 * y + qh), 8), pl.ds(128 * c, 128)]
                    t = pltpu.roll(t, (24 * g - 128 * j - 24 * pp) % 128, 1)
                    v = t if v is None else jnp.where(lane >= 24 * g - 128 * j, t, v)
                out[zm, pp, qh, j] = v


def z_backward(g, v, zi, acc, flow):
    table = cat([zi[g, 0], zi[g, 0], zi[g, 1]], 1)
    for j in (0, 2, 4, 6):
        n = min(2, 7 - j)
        rhs = cat([v[:, 2 * g : 2 * g + 2, j + i].reshape(128, 128) for i in range(n)], 1)
        hi, lo = split(rhs)
        part = dot(table, cat([hi, lo, hi], 0))
        ls = pl.ds(128 * j, 128 * n)
        if g == 0:
            acc[:, ls] = part
        elif g == 1:
            acc[:, ls] = acc[:, ls] + part
        else:
            flow[ls, :] = (acc[:, ls] + part).T


def far_first(i):
    return (2 + i + i // 2 + 2 * (i // 3)) % 4


def flow_kernel(
    vort, zf_h, yf_h, xf_h, xi_h, yi_h, zi_h,
    flow, xr, yr,
    zf, yf, xf, xi, yi, zi, w, zt, rv, yt, th, ub, uo, bk, vv, gt, s, o, f, u, acc, xs,
    tsem, osem, fs, fr, bs, br, d1, d2, hs,
):
    p, q = lax.axis_index("px"), lax.axis_index("py")
    core, half, qc = q % 2, p // 4, q // 2
    other = q + 1 - 2 * core
    mz, my, mx = p % 4, 2 * half + q // 8, qc % 4
    chip = p * 8 + qc
    own = half == core
    loads = [
        pltpu.make_async_copy(a, b, tsem.at[i])
        for i, (a, b) in enumerate([(zf_h, zf), (yf_h, yf), (xf_h, xf), (xi_h, xi), (yi_h, yi), (zi_h, zi)])
    ]
    for cp in loads:
        cp.start()

    near = [(p > 0, (p - 1, q)), (p < 7, (p + 1, q)), (q > 0, (p, q - 1)), (q < 15, (p, q + 1))]
    bar = pltpu.get_barrier_semaphore()

    def greet(i, _):
        pl.semaphore_signal(bar, inc=1, device_id=(core * 4 + i // 16, i % 16), device_id_type=MESH)
        return 0

    lax.fori_loop(0, 64, greet, 0)
    pl.semaphore_signal(bar, inc=1, device_id=(p, other), device_id_type=MESH)
    for has, dev in near:
        @pl.when(has)
        def _(dev=dev):
            pl.semaphore_signal(bar, inc=1, device_id=dev, device_id_type=MESH)

    loads[0].wait()
    z_forward(vort, zf, zt.reshape(8, 6, 7, 8, 128), w)
    pl.semaphore_wait(bar, 65 + sum(has.astype(jnp.int32) for has, _ in near))

    def forward(i, _):
        g, n = i // 64, i % 64
        x, y, z = (mx + far_first(n // 16)) % 4, (my + far_first((n // 4) % 4)) % 4, (mz + far_first(n % 4)) % 4
        a, b = (y // 2) * 4 + z, (y % 2) * 4 + x
        sr = zt.at[a, pl.ds(2 * g, 2), :, b]
        ds = rv.at[pl.ds(2 * g, 2), p % 4, q // 8, :, q % 8]
        me = jnp.logical_and(n == 63, own)

        @pl.when(me)
        def _():
            pltpu.make_async_copy(sr, ds, fr.at[g]).start()

        @pl.when(jnp.logical_not(me))
        def _():
            pltpu.make_async_remote_copy(sr, ds, fs, fr.at[g], device_id=(a, 2 * b + half), device_id_type=MESH).start()

        return 0

    lax.fori_loop(0, 192, forward, 0)
    green_table(chip, core, gt)

    rows_in = rv.reshape(6, 4, 2, 7, 8, 128)
    rows_out = bk.reshape(6, 4, 2, 7, 8, 128)

    def swap1(g):
        return pltpu.make_async_remote_copy(
            yt.at[1 - core, pl.ds(6 * g, 6)], th.at[pl.ds(6 * g, 6)], d1.at[0, g], d1.at[1, g],
            device_id=(p, other), device_id_type=MESH,
        )

    def swap2(g):
        return pltpu.make_async_remote_copy(
            uo.at[pl.ds(6 * g, 6)], ub.at[core, pl.ds(6 * g, 6)], d2.at[0, g], d2.at[1, g],
            device_id=(p, other), device_id_type=MESH,
        )

    def arrive(g):
        t = rv.at[pl.ds(2 * g, 2)]
        pltpu.make_async_copy(t, t, fr.at[g]).wait()

        def one(t, _):
            y_forward(2 * g + t, rows_in, yf, yt, s)
            return 0

        lax.fori_loop(0, 2, one, 0)
        swap1(g).start()

    for cp in loads[1:]:
        cp.wait()
    arrive(0)

    def group(g, _):
        swap1(g).wait_recv()
        x_stage(g, chip, core, yt, th, xf, xi, gt, ub, uo, f, u)
        swap2(g).start()

        @pl.when(g < 2)
        def _():
            arrive(g + 1)

        swap2(g).wait_recv()

        def one(t, _):
            y_backward(2 * g + t, ub, yi, rows_out, o)
            return 0

        lax.fori_loop(0, 2, one, 0)

        def backward(n, _):
            x, z = (mx + far_first(n // 16)) % 4, (mz + far_first((n // 4) % 4)) % 4
            yl, cr = (q // 8 + 1 + (n // 2) % 2) % 2, (core + 1 + n % 2) % 2
            a, b = core * 4 + z, yl * 8 + 2 * x + cr
            sr = bk.at[pl.ds(2 * g, 2), z, b // 8, :, b % 8]
            ds = vv.at[p, pl.ds(2 * g, 2), :, qc]
            me = jnp.logical_and(n == 63, own)

            @pl.when(me)
            def _():
                pltpu.make_async_copy(sr, ds, br.at[g]).start()

            @pl.when(jnp.logical_not(me))
            def _():
                pltpu.make_async_remote_copy(sr, ds, bs, br.at[g], device_id=(a, b), device_id_type=MESH).start()

            return 0

        lax.fori_loop(0, 64, backward, 0)
        return 0

    lax.fori_loop(0, 3, group, 0)

    vin = vv.reshape(8, 6, 7, 8, 128)
    for g in range(3):
        t = vv.at[:, pl.ds(2 * g, 2)]
        pltpu.make_async_copy(t, t, br.at[g]).wait()
        z_backward(g, vin, zi, acc, flow)

    for m in range(9):
        for e, r0 in ((0, 0), (1, 22)):
            for i in range(4):
                xs[e, m, pl.ds(2 * i, 2), :] = flow[pl.ds(24 * (4 * m + i) + r0, 2), :]
    srcs = [xs.at[0], xs.at[1], flow.at[pl.ds(0, 144)], flow.at[pl.ds(720, 144)]]
    dsts = [xr.at[1], xr.at[0], yr.at[1], yr.at[0]]
    back = [1, 0, 3, 2]
    cps = []
    for k, (has, dev) in enumerate(near):
        cps.append(pltpu.make_async_remote_copy(srcs[k], dsts[k], hs.at[0, k], hs.at[1, k], device_id=dev, device_id_type=MESH))

        @pl.when(has)
        def _(k=k):
            cps[k].start()

    ends = [xr.at[0], xr.at[1], yr.at[0], yr.at[1]]
    for k, ref in enumerate(ends):
        @pl.when(jnp.logical_not(near[k][0]))
        def _(ref=ref):
            ref[...] = jnp.zeros(ref.shape, f32)

    for g in range(3):
        swap1(g).wait_send()
        swap2(g).wait_send()
    flat = [zt.reshape(2688, 1, 128), bk.reshape(2688, 1, 128)]
    for n, cond in ((63, own), (64, jnp.logical_not(own))):
        @pl.when(cond)
        def _(n=n):
            for ref, sem in zip(flat, (fs, bs)):
                t = ref.at[pl.ds(0, 42 * n)]
                pltpu.make_async_copy(t, t, sem).wait()

    for k, (has, dev) in enumerate(near):
        @pl.when(has)
        def _(k=k):
            cps[k].wait_send()
            cps[back[k]].wait_recv()


def stretch_kernel(vort, flow, xr, yr, vel, st, pad):
    for i in range(36):
        pad[i, pl.ds(8, 24), :] = flow[pl.ds(24 * i, 24), :]
        pad[i, pl.ds(6, 2), :] = xr[0, i // 4, pl.ds(2 * (i % 4), 2), :]
        pad[i, pl.ds(32, 2), :] = xr[1, i // 4, pl.ds(2 * (i % 4), 2), :]

    def at_y(y, c):
        if y < 0:
            return yr[0, pl.ds(((y + 2) * 3 + c) * 24, 24), :]
        if y >= 12:
            return yr[1, pl.ds(((y - 12) * 3 + c) * 24, 24), :]
        return flow[pl.ds(24 * (3 * y + c), 24), :]

    def diff(m2, m1, p1, p2):
        return (8.0 * (p1 - m1) - (p2 - m2)) * (1.0 / 12.0)

    lane = lanes((24, 128))

    def put(out, c, yp, t):
        (a0, b0), (a1, b1) = [(v[:, :128], v[:, 128:]) for v in t]
        ra, rb = pltpu.roll(a1, 64, 1), pltpu.roll(b1, 64, 1)
        out[c, :, pl.ds(384 * yp, 128)] = a0
        out[c, :, pl.ds(384 * yp + 128, 128)] = jnp.where(lane < 64, b0, ra)
        out[c, :, pl.ds(384 * yp + 256, 128)] = jnp.where(lane < 64, ra, rb)

    for yp in range(6):
        fields = [[cat(padded_line(vort, d, 2 * yp + e, lane), 1) for d in range(3)] for e in range(2)]
        for c in range(3):
            t, vs = [], []
            for e in range(2):
                y = 2 * yp + e
                i = 3 * y + c
                wv = fields[e]
                dx = diff(*[pad[i, pl.ds(8 + k, 24), :] for k in (-2, -1, 1, 2)])
                dy = diff(*[at_y(y + k, c) for k in (-2, -1, 1, 2)])
                cur = at_y(y, c)
                dz = diff(*[pltpu.roll(cur, (-k) % 256, 1) for k in (-2, -1, 1, 2)])
                t.append(wv[0] * dx + wv[1] * dy + wv[2] * dz)
                vs.append(cur)
            put(vel, c, yp, vs)
            put(st, c, yp, t)


def sds(*shape):
    return jax.ShapeDtypeStruct(shape, f32)


def on_device(tb, vort):
    vspec, aspec = pl.BlockSpec(memory_space=VMEM), pl.BlockSpec(memory_space=ANY)
    dma = pltpu.SemaphoreType.DMA
    flow, xr, yr = pl.pallas_call(
        flow_kernel,
        out_shape=[sds(896, 256), sds(2, 9, 8, 256), sds(2, 144, 256)],
        in_specs=[vspec] + [aspec] * 6,
        out_specs=[vspec] * 3,
        scratch_shapes=[VMEM(t.shape, bf16) for t in tb]
        + [
            VMEM((896, 256), f32), VMEM((8, 6, 7, 8, 1, 128), f32), VMEM((6, 4, 2, 7, 8, 1, 128), f32),
            VMEM((2, 18, 192, 128), f32), VMEM((18, 192, 128), f32), VMEM((2, 18, 192, 128), f32),
            VMEM((18, 192, 128), f32), VMEM((6, 4, 2, 7, 8, 1, 128), f32), VMEM((8, 6, 7, 8, 1, 128), f32),
            VMEM((288, 384), f32), VMEM((192, 384), f32), VMEM((192, 384), f32),
            VMEM((2, 576, 384), f32), VMEM((2, 576, 384), f32), VMEM((256, 896), f32), VMEM((2, 9, 8, 256), f32),
            dma((6,)), dma((2,)), dma, dma((3,)), dma, dma((3,)), dma((2, 3)), dma((2, 3)), dma((2, 4)),
        ],
        compiler_params=pltpu.CompilerParams(collective_id=0, has_side_effects=True, vmem_limit_bytes=62 * 1024 * 1024),
    )(vort, *tb)
    return pl.pallas_call(
        stretch_kernel,
        out_shape=[sds(3, 24, 2304), sds(3, 24, 2304)],
        in_specs=[vspec] * 4,
        out_specs=[vspec] * 2,
        scratch_shapes=[VMEM((36, 40, 256), f32)],
        compiler_params=pltpu.CompilerParams(vmem_limit_bytes=40 * 1024 * 1024),
    )(vort, flow, xr, yr)


def solution(mesh):
    tb = [jnp.asarray(v) for v in tables()]
    return jax.shard_map(
        functools.partial(on_device, tb), mesh=mesh, in_specs=(P(None, "px", "py"),),
        out_specs=(P(None, "px", "py"), P(None, "px", "py")), check_vma=False,
    )
```

```python
import math
import functools
import itertools

import numpy as np
import jax
import jax.numpy as jnp
from jax import lax
from jax.experimental import pallas as pl
from jax.experimental.pallas import tpu as pltpu
from jax.sharding import PartitionSpec as P

G = 192
N = 2 * G
MESH = pl.DeviceIdType.MESH
VMEM = pltpu.VMEM
ANY = pl.ANY
bf16 = jnp.bfloat16
f32 = jnp.float32


def pair_np(t):
    hi = np.asarray(t, np.float32).astype(jnp.bfloat16)
    lo = (t - hi.astype(np.float64)).astype(np.float32).astype(jnp.bfloat16)
    return hi, lo


def trig(m, t, j):
    a = 2.0 * np.pi * ((m * j) % N) / N
    return np.where(t == 0, np.cos(a), np.sin(a))


def weight(m):
    return np.where(m == 0, 1.0, 2.0) / N


def tables():
    r = np.arange(384)
    dg, zm, dl = r // 48, (r // 8) % 6, r % 8
    mz, tz = 3 * (8 * dg + dl) + zm // 2, zm % 2
    z = np.arange(256)
    zf = np.where(z[None] < G, trig(mz[:, None], tz[:, None], z[None]), 0.0)
    zi = (zf * weight(mz)[:, None]).T.reshape(256, 8, 3, 2, 8).transpose(2, 0, 1, 3, 4).reshape(3, 256, 128)
    my, ty = 2 * (r % 96) + r // 192, (r // 96) % 2
    k = np.arange(192)
    jy = 12 * (k % 16) + k // 16
    yf = trig(my[:, None], ty[:, None], jy[None])
    yi = (yf * weight(my)[:, None]).T
    mx, tx = 64 * (r // 128) + r % 64, (r // 64) % 2
    lane = np.arange(128)
    jx = 24 * (2 * (lane[None] // 24) + np.arange(2)[:, None]) + lane[None] % 24
    xf = np.where(lane[None, :, None] < 96, trig(mx[None, None], tx[None, None], jx[:, :, None]), 0.0)
    xi = np.swapaxes(xf * weight(mx)[None, None], 1, 2)
    stack = lambda t: np.stack(pair_np(t), axis=-3)
    wide = lambda t: np.concatenate([pair_np(t)[0], pair_np(t)[0], pair_np(t)[1]], axis=-1)
    return [stack(zf), wide(yf), stack(xf), stack(xi), wide(yi), stack(zi)]


def split(x):
    hi = x.astype(bf16)
    lo = (x - hi.astype(f32)).astype(bf16)
    return hi, lo


def cat(parts, axis):
    return jnp.concatenate(parts, axis=axis)


def lanes(shape):
    return lax.broadcasted_iota(jnp.int32, shape, len(shape) - 1)


def dot(a, b, rhs_t=False):
    return lax.dot_general(a, b, (((1,), (1 if rhs_t else 0,)), ((), ())), preferred_element_type=f32)


def padded_line(vort, c, y, lane):
    a, b, d = [vort[c, :, pl.ds(384 * (y // 2) + 128 * i, 128)] for i in range(3)]
    if y % 2 == 0:
        return a, jnp.where(lane < 64, b, 0.0)
    rb, rd = pltpu.roll(b, 64, 1), pltpu.roll(d, 64, 1)
    return jnp.where(lane < 64, rb, rd), jnp.where(lane < 64, rd, 0.0)


def z_forward(vort, zf, out, w):
    lane = lanes((24, 128))
    for y in range(12):
        for c in range(3):
            v0, v1 = padded_line(vort, c, y, lane)
            r0 = y * 72 + c * 24
            w[pl.ds(r0, 24), pl.ds(0, 128)] = v0
            w[pl.ds(r0, 24), pl.ds(128, 128)] = v1
    w[pl.ds(864, 32), :] = jnp.zeros((32, 256), f32)
    table = cat([zf[0], zf[0], zf[1]], 1)
    for blk, n in ((0, 256), (256, 256), (512, 256), (768, 128)):
        hi, lo = split(w[pl.ds(blk, n), :])
        acc = dot(table, cat([hi, lo, hi], 1), rhs_t=True)
        for jj in range(n // 128):
            out[:, :, blk // 128 + jj] = acc[:, 128 * jj : 128 * jj + 128].reshape(8, 6, 8, 128)


def y_forward(g, h2, r, ty, out, s):
    zm = 2 * g + h2
    lane = lanes((8, 128))
    zero = jnp.zeros((8, 128), f32)
    for y in range(12):
        for c in range(3):
            j, o = divmod(24 * (3 * y + c), 128)
            for qh in range(2):
                v = zero
                for pp in (3, 2, 1, 0):
                    t = r[g, pp, qh, h2, j]
                    if o + 24 > 128:
                        t = jnp.where(lane >= o, t, r[g, pp, qh, h2, j + 1])
                    t = pltpu.roll(t, (24 * pp - o) % 128, 1)
                    v = jnp.where(lane < 24 * pp + 24, t, v)
                s[pl.ds(8 * (2 * y + qh), 8), pl.ds(128 * c, 128)] = v
    hi, lo = split(s[...])
    acc = dot(ty[...], cat([hi, lo, hi], 0))
    for h in range(2):
        for c in range(3):
            out[h, 3 * zm + c] = acc[192 * h : 192 * h + 192, 128 * c : 128 * c + 128]


def green_table(chip, core, out):
    unit = 2.0 * math.pi / N
    lane = lanes((8, 128))
    row = lax.broadcasted_iota(jnp.int32, (8, 128), 0)

    def body(it, _):
        kz = (3 * chip + it // 12).astype(f32) * unit
        ky = (16 * (it % 12) + core + 2 * row).astype(f32) * unit
        for tl in range(3):
            kx = (64 * tl + lane % 64).astype(f32) * unit
            sq = kx * kx + ky * ky + kz * kz
            green = jnp.exp(-0.5 * sq) / (sq + jnp.where(sq == 0.0, 1.0, 0.0))
            out[pl.ds(pl.multiple_of(8 * it, 8), 8), pl.ds(128 * tl, 128)] = green
        return 0

    lax.fori_loop(0, 36, body, 0)


B = 48


def x_stage(g, chip, core, yt, th, xf, xi, gt, ub, uo, f, u):
    unit = 2.0 * math.pi / N
    lane = lanes((8, 128))
    row = lax.broadcasted_iota(jnp.int32, (8, 128), 0)
    sign = jnp.where(lane < 64, 1.0, -1.0)
    kz = (3 * chip + g).astype(f32) * unit
    combos = [(t, c, s) for t in range(2) for c in range(3) for s in range(2)]
    at = lambda t, c, s: ((t * 3 + c) * 2 + s) * B
    tf = cat([xf[core, 0], xf[1 - core, 0], xf[core, 0], xf[1 - core, 0], xf[core, 1], xf[1 - core, 1]], 0)
    for ib in range(2):
        parts = []
        for t, c, s in combos:
            rows = pl.ds(96 * s + B * ib, B)
            zmc = 6 * g + 3 * t + c
            parts.append(cat([yt[core, zmc, rows, :], th[zmc, rows, :]], 1))
        hi, lo = split(cat(parts, 0))
        f[ib] = dot(cat([hi, lo, hi], 1), tf)
    for ib in range(2):
        for rt in range(B // 8):
            i0 = B * ib + 8 * rt
            ky = (2 * i0 + core + 2 * row).astype(f32) * unit
            for tl in range(3):
                kxs = (64 * tl + lane % 64).astype(f32) * unit * sign
                ls = pl.ds(128 * tl, 128)
                green = gt[pl.ds(pl.multiple_of(96 * g + i0, 8), 8), ls]
                pt = {k: f[ib, pl.ds(at(*k) + 8 * rt, 8), ls] * green for k in combos}
                for t in range(2):
                    dz = lambda c, s: (kz if t == 0 else -kz) * pt[1 - t, c, s]
                    for s in range(2):
                        dy = lambda c: (ky if s == 0 else -ky) * pt[t, c, 1 - s]
                        dx = lambda c: kxs * pltpu.roll(pt[t, c, s], 64, 1)
                        u[ib, pl.ds(at(t, 0, s) + 8 * rt, 8), ls] = dy(2) - dz(1, s)
                        u[ib, pl.ds(at(t, 1, s) + 8 * rt, 8), ls] = dz(0, s) - dx(2)
                        u[ib, pl.ds(at(t, 2, s) + 8 * rt, 8), ls] = dx(1) - dy(0)
    k0 = cat([xi[core, 0], xi[1 - core, 0]], 1)
    k1 = cat([xi[core, 1], xi[1 - core, 1]], 1)
    ti = cat([k0, k0, k1], 0)
    for ib in range(2):
        hi, lo = split(u[ib])
        back = dot(cat([hi, lo, hi], 1), ti)
        for t, c, s in combos:
            rows = pl.ds(96 * s + B * ib, B)
            zmc = 6 * g + 3 * t + c
            r0 = at(t, c, s)
            ub[core, zmc, rows, :] = back[r0 : r0 + B, :128]
            uo[zmc, rows, :] = back[r0 : r0 + B, 128:]


def y_backward(g, h2, ub, ty, out, o):
    zm = 2 * g + h2
    lane = lanes((8, 128))
    rhs = cat([cat([ub[h, 3 * zm + c] for c in range(3)], 1) for h in range(2)], 0)
    hi, lo = split(rhs)
    o[...] = dot(ty[...], cat([hi, lo, hi], 0))
    for pp in range(4):
        for qh in range(2):
            for j in range(7):
                v = None
                for i in range((128 * j) // 24, min((128 * j + 127) // 24, 35) + 1):
                    y, c = divmod(i, 3)
                    t = o[pl.ds(8 * (2 * y + qh), 8), pl.ds(128 * c, 128)]
                    t = pltpu.roll(t, (24 * i - 128 * j - 24 * pp) % 128, 1)
                    v = t if v is None else jnp.where(lane >= 24 * i - 128 * j, t, v)
                out[g, pp, qh, h2, j] = v


def z_backward(g, v, zi, acc, flow):
    table = cat([zi[g, 0], zi[g, 0], zi[g, 1]], 1)
    for j in (0, 2, 4, 6):
        n = min(2, 7 - j)
        rhs = cat([v[:, 2 * g : 2 * g + 2, j + i].reshape(128, 128) for i in range(n)], 1)
        hi, lo = split(rhs)
        part = dot(table, cat([hi, lo, hi], 0))
        ls = pl.ds(128 * j, 128 * n)
        if g == 0:
            acc[:, ls] = part
        elif g == 1:
            acc[:, ls] = acc[:, ls] + part
        else:
            flow[ls, :] = (acc[:, ls] + part).T


def hops(offset):
    return sum(min(v, 4 - v) for v in offset)


OFFSETS = sorted(itertools.product((2, 1, 3, 0), repeat=3), key=hops, reverse=True)
HALF = [d for d in OFFSETS if d[2] % 2 == 0]


def flow_kernel(
    vort_h, zf_h, yf_h, xf_h, xi_h, yi_h, zi_h,
    flow, xr, yr,
    zf, yf, xf, xi, yi, zi, vort, w, zt, rv, yt, th, ub, uo, bk, vv, gt, s, o, f, u, acc, xs,
    tsem, fs, fr, bs, br, d1, d2, hs,
):
    p, q = lax.axis_index("px"), lax.axis_index("py")
    core, half, qc = q % 2, p % 2, q // 2
    other = q + 1 - 2 * core
    mz, my, mx = p % 4, 2 * (p // 4) + q // 8, qc % 4
    chip = p * 8 + qc
    own = half == core
    loads = [
        pltpu.make_async_copy(a, b, tsem.at[i])
        for i, (a, b) in enumerate([(vort_h, vort), (zf_h, zf), (yf_h, yf), (xf_h, xf), (xi_h, xi), (yi_h, yi), (zi_h, zi)])
    ]
    for cp in loads:
        cp.start()

    near = [(p > 0, (p - 1, q)), (p < 7, (p + 1, q)), (q > 0, (p, q - 1)), (q < 15, (p, q + 1))]
    bar = pltpu.get_barrier_semaphore()

    for i in range(64):
        pl.semaphore_signal(bar, inc=1, device_id=(2 * (i // 16) + core, i % 16), device_id_type=MESH)
    pl.semaphore_signal(bar, inc=1, device_id=(p, other), device_id_type=MESH)
    for has, dev in near:
        @pl.when(has)
        def _(dev=dev):
            pl.semaphore_signal(bar, inc=1, device_id=dev, device_id_type=MESH)

    loads[0].wait()
    loads[1].wait()
    z_forward(vort, zf, zt.reshape(8, 6, 7, 8, 128), w)
    pl.semaphore_wait(bar, 65 + sum(has.astype(jnp.int32) for has, _ in near))

    def send(cond, sr, ds, ssem, rsem, dev):
        remote = pltpu.make_async_remote_copy(sr, ds, ssem, rsem, device_id=dev, device_id_type=MESH)
        if cond is None:
            remote.start()
            return

        @pl.when(cond)
        def _():
            pltpu.make_async_copy(sr, ds, rsem).start()

        @pl.when(jnp.logical_not(cond))
        def _():
            remote.start()

    def forward(g, _):
        ds = rv.at[g, p // 2, q // 8, :, :, q % 8]
        for dx, dy, dz in OFFSETS:
            x, y, z = (mx + dx) % 4, (my + dy) % 4, (mz + dz) % 4
            a, b = (y // 2) * 4 + z, (y % 2) * 4 + x
            last = own if (dx, dy, dz) == (0, 0, 0) else None
            send(last, zt.at[a, pl.ds(2 * g, 2), :, b], ds, fs, fr.at[g], (a, 2 * b + half))
        return 0

    lax.fori_loop(0, 3, forward, 0)
    green_table(chip, core, gt)

    rows_in = rv.reshape(3, 4, 2, 2, 7, 8, 128)
    rows_out = bk.reshape(3, 4, 2, 2, 7, 8, 128)

    def swap1(g, t):
        rows = pl.ds(6 * g + 3 * t, 3)
        return pltpu.make_async_remote_copy(
            yt.at[1 - core, rows], th.at[rows], d1.at[0, g, t], d1.at[1, g, t],
            device_id=(p, other), device_id_type=MESH,
        )

    def swap2(g):
        return pltpu.make_async_remote_copy(
            uo.at[pl.ds(6 * g, 6)], ub.at[core, pl.ds(6 * g, 6)], d2.at[0, g], d2.at[1, g],
            device_id=(p, other), device_id_type=MESH,
        )

    def arrive(g):
        t = rv.at[g]
        pltpu.make_async_copy(t, t, fr.at[g]).wait()

        def one(t, _):
            y_forward(g, t, rows_in, yf, yt, s)
            swap1(g, t).start()
            return 0

        lax.fori_loop(0, 2, one, 0)

    for cp in loads[2:]:
        cp.wait()
    arrive(0)

    def group(g, _):
        swap1(g, 0).wait_recv()
        swap1(g, 1).wait_recv()
        x_stage(g, chip, core, yt, th, xf, xi, gt, ub, uo, f, u)
        swap2(g).start()

        @pl.when(g < 2)
        def _():
            arrive(g + 1)

        swap2(g).wait_recv()

        def one(t, _):
            y_backward(g, t, ub, yi, rows_out, o)
            return 0

        lax.fori_loop(0, 2, one, 0)

        ds = vv.at[p, pl.ds(2 * g, 2), :, qc]
        for dx, dy, dz in HALF:
            x, y, z = (mx + dx) % 4, (my + dy) % 4, (mz + dz + (half + core) % 2) % 4
            for dc in (1, 0):
                a, b = (y // 2) * 4 + z, (y % 2) * 8 + 2 * x + (core + dc) % 2
                last = own if (dx, dy, dz, dc) == (0, 0, 0, 0) else None
                send(last, bk.at[g, a // 2, b // 8, :, :, b % 8], ds, bs, br.at[g], (a, b))
        return 0

    lax.fori_loop(0, 3, group, 0)

    vin = vv.reshape(8, 6, 7, 8, 128)
    for g in range(3):
        t = vv.at[:, pl.ds(2 * g, 2)]
        pltpu.make_async_copy(t, t, br.at[g]).wait()
        z_backward(g, vin, zi, acc, flow)

    for m in range(9):
        for e, r0 in ((0, 0), (1, 22)):
            for i in range(4):
                xs[e, m, pl.ds(2 * i, 2), :] = flow[pl.ds(24 * (4 * m + i) + r0, 2), :]
    srcs = [xs.at[0], xs.at[1], flow.at[pl.ds(0, 144)], flow.at[pl.ds(720, 144)]]
    dsts = [xr.at[1], xr.at[0], yr.at[1], yr.at[0]]
    back = [1, 0, 3, 2]
    cps = []
    for k, (has, dev) in enumerate(near):
        cps.append(pltpu.make_async_remote_copy(srcs[k], dsts[k], hs.at[0, k], hs.at[1, k], device_id=dev, device_id_type=MESH))

        @pl.when(has)
        def _(k=k):
            cps[k].start()

    ends = [xr.at[0], xr.at[1], yr.at[0], yr.at[1]]
    for k, ref in enumerate(ends):
        @pl.when(jnp.logical_not(near[k][0]))
        def _(ref=ref):
            ref[...] = jnp.zeros(ref.shape, f32)

    for g in range(3):
        swap1(g, 0).wait_send()
        swap1(g, 1).wait_send()
        swap2(g).wait_send()
    flat = [zt.reshape(2688, 1, 128), bk.reshape(2688, 1, 128)]
    for n, cond in ((63, own), (64, jnp.logical_not(own))):
        @pl.when(cond)
        def _(n=n):
            for ref, sem in zip(flat, (fs, bs)):
                t = ref.at[pl.ds(0, 42 * n)]
                pltpu.make_async_copy(t, t, sem).wait()

    for k, (has, dev) in enumerate(near):
        @pl.when(has)
        def _(k=k):
            cps[k].wait_send()
            cps[back[k]].wait_recv()


def stretch_kernel(vort, flow, xr, yr, vel, st, pad):
    for i in range(36):
        pad[i, pl.ds(8, 24), :] = flow[pl.ds(24 * i, 24), :]
        pad[i, pl.ds(6, 2), :] = xr[0, i // 4, pl.ds(2 * (i % 4), 2), :]
        pad[i, pl.ds(32, 2), :] = xr[1, i // 4, pl.ds(2 * (i % 4), 2), :]

    def at_y(y, c):
        if y < 0:
            return yr[0, pl.ds(((y + 2) * 3 + c) * 24, 24), :]
        if y >= 12:
            return yr[1, pl.ds(((y - 12) * 3 + c) * 24, 24), :]
        return flow[pl.ds(24 * (3 * y + c), 24), :]

    def diff(m2, m1, p1, p2):
        return (8.0 * (p1 - m1) - (p2 - m2)) * (1.0 / 12.0)

    lane = lanes((24, 128))

    def put(out, c, yp, t):
        (a0, b0), (a1, b1) = [(v[:, :128], v[:, 128:]) for v in t]
        ra, rb = pltpu.roll(a1, 64, 1), pltpu.roll(b1, 64, 1)
        out[c, :, pl.ds(384 * yp, 128)] = a0
        out[c, :, pl.ds(384 * yp + 128, 128)] = jnp.where(lane < 64, b0, ra)
        out[c, :, pl.ds(384 * yp + 256, 128)] = jnp.where(lane < 64, ra, rb)

    for yp in range(6):
        fields = [[cat(padded_line(vort, d, 2 * yp + e, lane), 1) for d in range(3)] for e in range(2)]
        for c in range(3):
            t, vs = [], []
            for e in range(2):
                y = 2 * yp + e
                i = 3 * y + c
                wv = fields[e]
                dx = diff(*[pad[i, pl.ds(8 + k, 24), :] for k in (-2, -1, 1, 2)])
                dy = diff(*[at_y(y + k, c) for k in (-2, -1, 1, 2)])
                cur = at_y(y, c)
                dz = diff(*[pltpu.roll(cur, (-k) % 256, 1) for k in (-2, -1, 1, 2)])
                t.append(wv[0] * dx + wv[1] * dy + wv[2] * dz)
                vs.append(cur)
            put(vel, c, yp, vs)
            put(st, c, yp, t)


def sds(*shape):
    return jax.ShapeDtypeStruct(shape, f32)


def on_device(tb, vort):
    vspec, aspec = pl.BlockSpec(memory_space=VMEM), pl.BlockSpec(memory_space=ANY)
    dma = pltpu.SemaphoreType.DMA
    flow, xr, yr = pl.pallas_call(
        flow_kernel,
        out_shape=[sds(896, 256), sds(2, 9, 8, 256), sds(2, 144, 256)],
        in_specs=[aspec] * 7,
        out_specs=[vspec] * 3,
        scratch_shapes=[VMEM(t.shape, bf16) for t in tb]
        + [
            VMEM((3, 24, 2304), f32), VMEM((896, 256), f32), VMEM((8, 6, 7, 8, 1, 128), f32), VMEM((3, 4, 2, 2, 7, 8, 1, 128), f32),
            VMEM((2, 18, 192, 128), f32), VMEM((18, 192, 128), f32), VMEM((2, 18, 192, 128), f32),
            VMEM((18, 192, 128), f32), VMEM((3, 4, 2, 2, 7, 8, 1, 128), f32), VMEM((8, 6, 7, 8, 1, 128), f32),
            VMEM((288, 384), f32), VMEM((192, 384), f32), VMEM((192, 384), f32),
            VMEM((2, 576, 384), f32), VMEM((2, 576, 384), f32), VMEM((256, 896), f32), VMEM((2, 9, 8, 256), f32),
            dma((7,)), dma, dma((3,)), dma, dma((3,)), dma((2, 3, 2)), dma((2, 3)), dma((2, 4)),
        ],
        compiler_params=pltpu.CompilerParams(collective_id=0, has_side_effects=True, vmem_limit_bytes=60 * 1024 * 1024),
    )(vort, *tb)
    return pl.pallas_call(
        stretch_kernel,
        out_shape=[sds(3, 24, 2304), sds(3, 24, 2304)],
        in_specs=[vspec] * 4,
        out_specs=[vspec] * 2,
        scratch_shapes=[VMEM((36, 40, 256), f32)],
        compiler_params=pltpu.CompilerParams(vmem_limit_bytes=61 * 1024 * 1024),
    )(vort, flow, xr, yr)


def solution(mesh):
    tb = [jnp.asarray(v) for v in tables()]
    return jax.shard_map(
        functools.partial(on_device, tb), mesh=mesh, in_specs=(P(None, "px", "py"),),
        out_specs=(P(None, "px", "py"), P(None, "px", "py")), check_vma=False,
    )
```

```python
import math
import functools
import itertools

import numpy as np
import jax
import jax.numpy as jnp
from jax import lax
from jax.experimental import pallas as pl
from jax.experimental.pallas import tpu as pltpu
from jax.sharding import PartitionSpec as P

G = 192
N = 2 * G
MESH = pl.DeviceIdType.MESH
VMEM = pltpu.VMEM
ANY = pl.ANY
bf16 = jnp.bfloat16
f32 = jnp.float32


def pair_np(t):
    hi = np.asarray(t, np.float32).astype(jnp.bfloat16)
    lo = (t - hi.astype(np.float64)).astype(np.float32).astype(jnp.bfloat16)
    return hi, lo


def trig(m, t, j):
    a = 2.0 * np.pi * ((m * j) % N) / N
    return np.where(t == 0, np.cos(a), np.sin(a))


def weight(m):
    return np.where(m == 0, 1.0, 2.0) / N


def tables():
    r = np.arange(384)
    dg, zm, dl = r // 48, (r // 8) % 6, r % 8
    mz, tz = 3 * (8 * dg + dl) + zm // 2, zm % 2
    z = np.arange(256)
    zf = np.where(z[None] < G, trig(mz[:, None], tz[:, None], z[None]), 0.0)
    zi = (zf * weight(mz)[:, None]).T.reshape(256, 8, 3, 2, 8).transpose(2, 0, 1, 3, 4).reshape(3, 256, 128)
    my, ty = 2 * (r % 96) + r // 192, (r // 96) % 2
    k = np.arange(192)
    jy = 12 * (k % 16) + k // 16
    yf = trig(my[:, None], ty[:, None], jy[None])
    yi = (yf * weight(my)[:, None]).T
    mx, tx = 64 * (r // 128) + r % 64, (r // 64) % 2
    lane = np.arange(128)
    jx = 24 * (2 * (lane[None] // 24) + np.arange(2)[:, None]) + lane[None] % 24
    xf = np.where(lane[None, :, None] < 96, trig(mx[None, None], tx[None, None], jx[:, :, None]), 0.0)
    xi = np.swapaxes(xf * weight(mx)[None, None], 1, 2)
    stack = lambda t: np.stack(pair_np(t), axis=-3)
    wide = lambda t: np.concatenate([pair_np(t)[0], pair_np(t)[0], pair_np(t)[1]], axis=-1)
    return [stack(zf), wide(yf), stack(xf), stack(xi), wide(yi), stack(zi)]


def split(x):
    hi = x.astype(bf16)
    lo = (x - hi.astype(f32)).astype(bf16)
    return hi, lo


def cat(parts, axis):
    return jnp.concatenate(parts, axis=axis)


def lanes(shape):
    return lax.broadcasted_iota(jnp.int32, shape, len(shape) - 1)


def dot(a, b, rhs_t=False):
    return lax.dot_general(a, b, (((1,), (1 if rhs_t else 0,)), ((), ())), preferred_element_type=f32)


def padded_line(vort, c, y, lane):
    a, b, d = [vort[c, :, pl.ds(384 * (y // 2) + 128 * i, 128)] for i in range(3)]
    if y % 2 == 0:
        return a, jnp.where(lane < 64, b, 0.0)
    rb, rd = pltpu.roll(b, 64, 1), pltpu.roll(d, 64, 1)
    return jnp.where(lane < 64, rb, rd), jnp.where(lane < 64, rd, 0.0)


def z_forward(vort, zf, out, w):
    lane = lanes((24, 128))
    for y in range(12):
        for c in range(3):
            v0, v1 = padded_line(vort, c, y, lane)
            r0 = y * 72 + c * 24
            w[pl.ds(r0, 24), pl.ds(0, 128)] = v0
            w[pl.ds(r0, 24), pl.ds(128, 128)] = v1
    w[pl.ds(864, 32), :] = jnp.zeros((32, 256), f32)
    table = cat([zf[0], zf[0], zf[1]], 1)
    for blk, n in ((0, 256), (256, 256), (512, 256), (768, 128)):
        hi, lo = split(w[pl.ds(blk, n), :])
        acc = dot(table, cat([hi, lo, hi], 1), rhs_t=True)
        for jj in range(n // 128):
            out[:, :, blk // 128 + jj] = acc[:, 128 * jj : 128 * jj + 128].reshape(8, 6, 8, 128)


def y_forward(g, h2, r, ty, out, s):
    zm = 2 * g + h2
    lane = lanes((8, 128))
    zero = jnp.zeros((8, 128), f32)
    for y in range(12):
        for c in range(3):
            j, o = divmod(24 * (3 * y + c), 128)
            for qh in range(2):
                v = zero
                for pp in (3, 2, 1, 0):
                    t = r[g, pp, qh, h2, j]
                    if o + 24 > 128:
                        t = jnp.where(lane >= o, t, r[g, pp, qh, h2, j + 1])
                    t = pltpu.roll(t, (24 * pp - o) % 128, 1)
                    v = jnp.where(lane < 24 * pp + 24, t, v)
                s[pl.ds(8 * (2 * y + qh), 8), pl.ds(128 * c, 128)] = v
    hi, lo = split(s[...])
    acc = dot(ty[...], cat([hi, lo, hi], 0))
    for h in range(2):
        for c in range(3):
            out[h, 3 * zm + c] = acc[192 * h : 192 * h + 192, 128 * c : 128 * c + 128]


def green_table(chip, core, out):
    unit = 2.0 * math.pi / N
    lane = lanes((8, 128))
    row = lax.broadcasted_iota(jnp.int32, (8, 128), 0)

    def body(it, _):
        kz = (3 * chip + it // 12).astype(f32) * unit
        ky = (16 * (it % 12) + core + 2 * row).astype(f32) * unit
        for tl in range(3):
            kx = (64 * tl + lane % 64).astype(f32) * unit
            sq = kx * kx + ky * ky + kz * kz
            green = jnp.exp(-0.5 * sq) / (sq + jnp.where(sq == 0.0, 1.0, 0.0))
            out[pl.ds(pl.multiple_of(8 * it, 8), 8), pl.ds(128 * tl, 128)] = green
        return 0

    lax.fori_loop(0, 36, body, 0)


B = 48


def x_stage(g, chip, core, yt, th, xf, xi, gt, ub, uo, f, u):
    unit = 2.0 * math.pi / N
    lane = lanes((8, 128))
    row = lax.broadcasted_iota(jnp.int32, (8, 128), 0)
    sign = jnp.where(lane < 64, 1.0, -1.0)
    kz = (3 * chip + g).astype(f32) * unit
    combos = [(t, c, s) for t in range(2) for c in range(3) for s in range(2)]
    at = lambda t, c, s: ((t * 3 + c) * 2 + s) * B
    tf = cat([xf[core, 0], xf[1 - core, 0], xf[core, 0], xf[1 - core, 0], xf[core, 1], xf[1 - core, 1]], 0)
    for ib in range(2):
        parts = []
        for t, c, s in combos:
            rows = pl.ds(96 * s + B * ib, B)
            zmc = 6 * g + 3 * t + c
            parts.append(cat([yt[core, zmc, rows, :], th[zmc, rows, :]], 1))
        hi, lo = split(cat(parts, 0))
        f[ib] = dot(cat([hi, lo, hi], 1), tf)
    for ib in range(2):
        for rt in range(B // 8):
            i0 = B * ib + 8 * rt
            ky = (2 * i0 + core + 2 * row).astype(f32) * unit
            for tl in range(3):
                kxs = (64 * tl + lane % 64).astype(f32) * unit * sign
                ls = pl.ds(128 * tl, 128)
                green = gt[pl.ds(pl.multiple_of(96 * g + i0, 8), 8), ls]
                pt = {k: f[ib, pl.ds(at(*k) + 8 * rt, 8), ls] * green for k in combos}
                for t in range(2):
                    dz = lambda c, s: (kz if t == 0 else -kz) * pt[1 - t, c, s]
                    for s in range(2):
                        dy = lambda c: (ky if s == 0 else -ky) * pt[t, c, 1 - s]
                        dx = lambda c: kxs * pltpu.roll(pt[t, c, s], 64, 1)
                        u[ib, pl.ds(at(t, 0, s) + 8 * rt, 8), ls] = dy(2) - dz(1, s)
                        u[ib, pl.ds(at(t, 1, s) + 8 * rt, 8), ls] = dz(0, s) - dx(2)
                        u[ib, pl.ds(at(t, 2, s) + 8 * rt, 8), ls] = dx(1) - dy(0)
    k0 = cat([xi[core, 0], xi[1 - core, 0]], 1)
    k1 = cat([xi[core, 1], xi[1 - core, 1]], 1)
    ti = cat([k0, k0, k1], 0)
    for ib in range(2):
        hi, lo = split(u[ib])
        back = dot(cat([hi, lo, hi], 1), ti)
        for t, c, s in combos:
            rows = pl.ds(96 * s + B * ib, B)
            zmc = 6 * g + 3 * t + c
            r0 = at(t, c, s)
            ub[core, zmc, rows, :] = back[r0 : r0 + B, :128]
            uo[zmc, rows, :] = back[r0 : r0 + B, 128:]


def y_backward(g, h2, ub, ty, out, o):
    zm = 2 * g + h2
    lane = lanes((8, 128))
    rhs = cat([cat([ub[h, 3 * zm + c] for c in range(3)], 1) for h in range(2)], 0)
    hi, lo = split(rhs)
    o[...] = dot(ty[...], cat([hi, lo, hi], 0))
    for pp in range(4):
        for qh in range(2):
            for j in range(7):
                v = None
                for i in range((128 * j) // 24, min((128 * j + 127) // 24, 35) + 1):
                    y, c = divmod(i, 3)
                    t = o[pl.ds(8 * (2 * y + qh), 8), pl.ds(128 * c, 128)]
                    t = pltpu.roll(t, (24 * i - 128 * j - 24 * pp) % 128, 1)
                    v = t if v is None else jnp.where(lane >= 24 * i - 128 * j, t, v)
                out[g, pp, qh, h2, j] = v


def z_backward(g, v, zi, acc, flow):
    table = cat([zi[g, 0], zi[g, 0], zi[g, 1]], 1)
    for j in (0, 2, 4, 6):
        n = min(2, 7 - j)
        rhs = cat([v[:, 2 * g : 2 * g + 2, j + i].reshape(128, 128) for i in range(n)], 1)
        hi, lo = split(rhs)
        part = dot(table, cat([hi, lo, hi], 0))
        ls = pl.ds(128 * j, 128 * n)
        if g == 0:
            acc[:, ls] = part
        elif g == 1:
            acc[:, ls] = acc[:, ls] + part
        else:
            flow[ls, :] = (acc[:, ls] + part).T


def diff(m2, m1, p1, p2):
    return (8.0 * (p1 - m1) - (p2 - m2)) * (1.0 / 12.0)


def put(out, c, yp, pair):
    lane = lanes((24, 128))
    (a0, b0), (a1, b1) = [(v[:, :128], v[:, 128:]) for v in pair]
    ra, rb = pltpu.roll(a1, 64, 1), pltpu.roll(b1, 64, 1)
    out[c, :, pl.ds(384 * yp, 128)] = a0
    out[c, :, pl.ds(384 * yp + 128, 128)] = jnp.where(lane < 64, b0, ra)
    out[c, :, pl.ds(384 * yp + 256, 128)] = jnp.where(lane < 64, ra, rb)


def inner_stretch(flow, w, part):
    row = lax.broadcasted_iota(jnp.int32, (24, 256), 0)
    zero = jnp.zeros((24, 256), f32)
    for y in range(12):
        for c in range(3):
            i = 3 * y + c
            line = lambda k: flow[pl.ds(24 * (3 * k + c), 24), :] if 0 <= k < 12 else zero
            cur = line(y)
            dx = diff(*[
                jnp.where(jnp.logical_and(row + k >= 0, row + k < 24), pltpu.roll(cur, (-k) % 24, 0), zero)
                for k in (-2, -1, 1, 2)
            ])
            dy = diff(*[line(y + k) for k in (-2, -1, 1, 2)])
            dz = diff(*[pltpu.roll(cur, (-k) % 256, 1) for k in (-2, -1, 1, 2)])
            wv = [w[pl.ds(72 * y + 24 * d, 24), :] for d in range(3)]
            part[pl.ds(24 * i, 24), :] = wv[0] * dx + wv[1] * dy + wv[2] * dz


def edge_stretch(w, part, xr, yr, top, low, st):
    zero = jnp.zeros((24, 256), f32)
    for i in range(36):
        top[i, pl.ds(6, 2), :] = xr[0, i // 4, pl.ds(2 * (i % 4), 2), :]
        low[i, pl.ds(10, 2), :] = xr[1, i // 4, pl.ds(2 * (i % 4), 2), :]
    for yp in range(6):
        for c in range(3):
            pair = []
            for y in (2 * yp, 2 * yp + 1):
                i = 3 * y + c
                v = part[pl.ds(24 * i, 24), :]
                wx = w[pl.ds(72 * y, 24), :]
                head = diff(*[top[i, pl.ds(8 + k, 8), :] for k in (-2, -1, 1, 2)])
                tail = diff(*[low[i, pl.ds(2 + k, 8), :] for k in (-2, -1, 1, 2)])
                v = cat([v[0:8] + wx[0:8] * head, v[8:16], v[16:24] + wx[16:24] * tail], 0)
                if y < 2 or y > 9:
                    def line(k):
                        if k < 0:
                            return yr[0, pl.ds(((k + 2) * 3 + c) * 24, 24), :]
                        return yr[1, pl.ds(((k - 12) * 3 + c) * 24, 24), :] if k >= 12 else zero

                    dy = diff(*[line(y + k) for k in (-2, -1, 1, 2)])
                    v = v + w[pl.ds(72 * y + 24, 24), :] * dy
                pair.append(v)
            put(st, c, yp, pair)


def hops(offset):
    return sum(min(v, 4 - v) for v in offset)


OFFSETS = sorted(itertools.product((2, 1, 3, 0), repeat=3), key=hops, reverse=True)
HALF = [d for d in OFFSETS if d[2] % 2 == 0]


def flow_kernel(
    vort_h, zf_h, yf_h, xf_h, xi_h, yi_h, zi_h,
    vel_h, st_h,
    zf, yf, xf, xi, yi, zi, vort, w, zt, rv, yt, th, ub, uo, bk, vv, gt, s, o, f, u, acc, xs,
    flow, xr, yr, vel, st, part, top, low,
    tsem, fs, fr, bs, br, d1, d2, hs, os,
):
    p, q = lax.axis_index("px"), lax.axis_index("py")
    core, half, qc = q % 2, p % 2, q // 2
    other = q + 1 - 2 * core
    mz, my, mx = p % 4, 2 * (p // 4) + q // 8, qc % 4
    chip = p * 8 + qc
    own = half == core
    loads = [
        pltpu.make_async_copy(a, b, tsem.at[i])
        for i, (a, b) in enumerate([(vort_h, vort), (zf_h, zf), (yf_h, yf), (xf_h, xf), (xi_h, xi), (yi_h, yi), (zi_h, zi)])
    ]
    for cp in loads:
        cp.start()

    near = [(p > 0, (p - 1, q)), (p < 7, (p + 1, q)), (q > 0, (p, q - 1)), (q < 15, (p, q + 1))]
    bar = pltpu.get_barrier_semaphore()

    for i in range(64):
        pl.semaphore_signal(bar, inc=1, device_id=(2 * (i // 16) + core, i % 16), device_id_type=MESH)
    pl.semaphore_signal(bar, inc=1, device_id=(p, other), device_id_type=MESH)
    for has, dev in near:
        @pl.when(has)
        def _(dev=dev):
            pl.semaphore_signal(bar, inc=1, device_id=dev, device_id_type=MESH)

    loads[0].wait()
    loads[1].wait()
    z_forward(vort, zf, zt.reshape(8, 6, 7, 8, 128), w)
    pl.semaphore_wait(bar, 65 + sum(has.astype(jnp.int32) for has, _ in near))

    def send(cond, sr, ds, ssem, rsem, dev):
        remote = pltpu.make_async_remote_copy(sr, ds, ssem, rsem, device_id=dev, device_id_type=MESH)
        if cond is None:
            remote.start()
            return

        @pl.when(cond)
        def _():
            pltpu.make_async_copy(sr, ds, rsem).start()

        @pl.when(jnp.logical_not(cond))
        def _():
            remote.start()

    def forward(g, _):
        ds = rv.at[g, p // 2, q // 8, :, :, q % 8]
        for dx, dy, dz in OFFSETS:
            x, y, z = (mx + dx) % 4, (my + dy) % 4, (mz + dz) % 4
            a, b = (y // 2) * 4 + z, (y % 2) * 4 + x
            last = own if (dx, dy, dz) == (0, 0, 0) else None
            send(last, zt.at[a, pl.ds(2 * g, 2), :, b], ds, fs, fr.at[g], (a, 2 * b + half))
        return 0

    lax.fori_loop(0, 3, forward, 0)
    green_table(chip, core, gt)
    top[...] = jnp.zeros(top.shape, f32)
    low[...] = jnp.zeros(low.shape, f32)

    rows_in = rv.reshape(3, 4, 2, 2, 7, 8, 128)
    rows_out = bk.reshape(3, 4, 2, 2, 7, 8, 128)

    def swap1(g, t):
        rows = pl.ds(6 * g + 3 * t, 3)
        return pltpu.make_async_remote_copy(
            yt.at[1 - core, rows], th.at[rows], d1.at[0, g, t], d1.at[1, g, t],
            device_id=(p, other), device_id_type=MESH,
        )

    def swap2(g):
        return pltpu.make_async_remote_copy(
            uo.at[pl.ds(6 * g, 6)], ub.at[core, pl.ds(6 * g, 6)], d2.at[0, g], d2.at[1, g],
            device_id=(p, other), device_id_type=MESH,
        )

    def arrive(g):
        t = rv.at[g]
        pltpu.make_async_copy(t, t, fr.at[g]).wait()

        def one(t, _):
            y_forward(g, t, rows_in, yf, yt, s)
            swap1(g, t).start()
            return 0

        lax.fori_loop(0, 2, one, 0)

    for cp in loads[2:]:
        cp.wait()
    arrive(0)

    def group(g, _):
        swap1(g, 0).wait_recv()
        swap1(g, 1).wait_recv()
        x_stage(g, chip, core, yt, th, xf, xi, gt, ub, uo, f, u)
        swap2(g).start()

        @pl.when(g < 2)
        def _():
            arrive(g + 1)

        swap2(g).wait_recv()

        def one(t, _):
            y_backward(g, t, ub, yi, rows_out, o)
            return 0

        lax.fori_loop(0, 2, one, 0)

        ds = vv.at[p, pl.ds(2 * g, 2), :, qc]
        for dc in (1, 0):
            for dx, dy, dz in HALF:
                x, y, z = (mx + dx) % 4, (my + dy) % 4, (mz + dz + (half + core) % 2) % 4
                a, b = (y // 2) * 4 + z, (y % 2) * 8 + 2 * x + (core + dc) % 2
                last = own if (dx, dy, dz, dc) == (0, 0, 0, 0) else None
                send(last, bk.at[g, a // 2, b // 8, :, :, b % 8], ds, bs, br.at[g], (a, b))
        return 0

    lax.fori_loop(0, 3, group, 0)

    vin = vv.reshape(8, 6, 7, 8, 128)
    for g in range(3):
        t = vv.at[:, pl.ds(2 * g, 2)]
        pltpu.make_async_copy(t, t, br.at[g]).wait()
        z_backward(g, vin, zi, acc, flow)

    for m in range(9):
        for e, r0 in ((0, 0), (1, 22)):
            for i in range(4):
                xs[e, m, pl.ds(2 * i, 2), :] = flow[pl.ds(24 * (4 * m + i) + r0, 2), :]
    srcs = [xs.at[0], xs.at[1], flow.at[pl.ds(0, 144)], flow.at[pl.ds(720, 144)]]
    dsts = [xr.at[1], xr.at[0], yr.at[1], yr.at[0]]
    back = [1, 0, 3, 2]
    cps = []
    for k, (has, dev) in enumerate(near):
        cps.append(pltpu.make_async_remote_copy(srcs[k], dsts[k], hs.at[0, k], hs.at[1, k], device_id=dev, device_id_type=MESH))

        @pl.when(has)
        def _(k=k):
            cps[k].start()

    ends = [xr.at[0], xr.at[1], yr.at[0], yr.at[1]]
    for k, ref in enumerate(ends):
        @pl.when(jnp.logical_not(near[k][0]))
        def _(ref=ref):
            ref[...] = jnp.zeros(ref.shape, f32)

    for yp in range(6):
        for c in range(3):
            put(vel, c, yp, [flow[pl.ds(24 * (3 * (2 * yp + e) + c), 24), :] for e in range(2)])
    out_vel = pltpu.make_async_copy(vel, vel_h, os.at[0])
    out_vel.start()
    inner_stretch(flow, w, part)

    for g in range(3):
        swap1(g, 0).wait_send()
        swap1(g, 1).wait_send()
        swap2(g).wait_send()
    flat = [zt.reshape(2688, 1, 128), bk.reshape(2688, 1, 128)]
    for n, cond in ((63, own), (64, jnp.logical_not(own))):
        @pl.when(cond)
        def _(n=n):
            for ref, sem in zip(flat, (fs, bs)):
                t = ref.at[pl.ds(0, 42 * n)]
                pltpu.make_async_copy(t, t, sem).wait()

    for k, (has, dev) in enumerate(near):
        @pl.when(has)
        def _(k=k):
            cps[k].wait_send()
            cps[back[k]].wait_recv()

    edge_stretch(w, part, xr, yr, top, low, st)
    out_st = pltpu.make_async_copy(st, st_h, os.at[1])
    out_st.start()
    out_vel.wait()
    out_st.wait()


def sds(*shape):
    return jax.ShapeDtypeStruct(shape, f32)


def on_device(tb, vort):
    vspec, aspec = pl.BlockSpec(memory_space=VMEM), pl.BlockSpec(memory_space=ANY)
    dma = pltpu.SemaphoreType.DMA
    vel, st = pl.pallas_call(
        flow_kernel,
        out_shape=[sds(3, 24, 2304)] * 2,
        in_specs=[aspec] * 7,
        out_specs=[aspec] * 2,
        scratch_shapes=[VMEM(t.shape, bf16) for t in tb]
        + [
            VMEM((3, 24, 2304), f32), VMEM((896, 256), f32), VMEM((8, 6, 7, 8, 1, 128), f32), VMEM((3, 4, 2, 2, 7, 8, 1, 128), f32),
            VMEM((2, 18, 192, 128), f32), VMEM((18, 192, 128), f32), VMEM((2, 18, 192, 128), f32),
            VMEM((18, 192, 128), f32), VMEM((3, 4, 2, 2, 7, 8, 1, 128), f32), VMEM((8, 6, 7, 8, 1, 128), f32),
            VMEM((288, 384), f32), VMEM((192, 384), f32), VMEM((192, 384), f32),
            VMEM((2, 576, 384), f32), VMEM((2, 576, 384), f32), VMEM((256, 896), f32), VMEM((2, 9, 8, 256), f32),
            VMEM((896, 256), f32), VMEM((2, 9, 8, 256), f32), VMEM((2, 144, 256), f32),
            VMEM((3, 24, 2304), f32), VMEM((3, 24, 2304), f32), VMEM((896, 256), f32),
            VMEM((36, 24, 256), f32), VMEM((36, 24, 256), f32),
            dma((7,)), dma, dma((3,)), dma, dma((3,)), dma((2, 3, 2)), dma((2, 3)), dma((2, 4)), dma((2,)),
        ],
        compiler_params=pltpu.CompilerParams(collective_id=0, has_side_effects=True, vmem_limit_bytes=60 * 1024 * 1024),
    )(vort, *tb)
    return pl.pallas_call(
        hand_over,
        out_shape=[sds(3, 24, 2304)] * 2,
        in_specs=[aspec] * 2,
        out_specs=[aspec] * 2,
        scratch_shapes=[VMEM((3, 24, 2304), f32), VMEM((3, 24, 2304), f32), dma((2, 2, 3))],
        compiler_params=pltpu.CompilerParams(vmem_limit_bytes=61 * 1024 * 1024),
    )(vel, st)


def hand_over(vel, st, vel_o, st_o, a, b, sem):
    triples = [(k, c, x, t, o) for k, (x, t, o) in enumerate(((vel, a, vel_o), (st, b, st_o))) for c in range(3)]
    ins = [pltpu.make_async_copy(x.at[c], t.at[c], sem.at[0, k, c]) for k, c, x, t, o in triples]
    outs = [pltpu.make_async_copy(t.at[c], o.at[c], sem.at[1, k, c]) for k, c, x, t, o in triples]
    for cp in ins:
        cp.start()
    for i, o in zip(ins, outs):
        i.wait()
        o.start()
    for cp in outs:
        cp.wait()


def solution(mesh):
    tb = [jnp.asarray(v) for v in tables()]
    return jax.shard_map(
        functools.partial(on_device, tb), mesh=mesh, in_specs=(P(None, "px", "py"),),
        out_specs=(P(None, "px", "py"), P(None, "px", "py")), check_vma=False,
    )
```

```python
import math
import functools
import itertools

import numpy as np
import jax
import jax.numpy as jnp
from jax import lax
from jax.experimental import pallas as pl
from jax.experimental.pallas import tpu as pltpu
from jax.sharding import PartitionSpec as P

G = 192
N = 2 * G
MESH = pl.DeviceIdType.MESH
VMEM = pltpu.VMEM
ANY = pl.ANY
bf16 = jnp.bfloat16
f32 = jnp.float32


def pair_np(t):
    hi = np.asarray(t, np.float32).astype(jnp.bfloat16)
    lo = (t - hi.astype(np.float64)).astype(np.float32).astype(jnp.bfloat16)
    return hi, lo


def trig(m, t, j):
    a = 2.0 * np.pi * ((m * j) % N) / N
    return np.where(t == 0, np.cos(a), np.sin(a))


def weight(m):
    return np.where(m == 0, 1.0, 2.0) / N


def tables():
    r = np.arange(384)
    dg, zm, dl = r // 48, (r // 8) % 6, r % 8
    mz, tz = 3 * (8 * dg + dl) + zm // 2, zm % 2
    z = np.arange(256)
    zf = np.where(z[None] < G, trig(mz[:, None], tz[:, None], z[None]), 0.0)
    zi = (zf * weight(mz)[:, None]).T.reshape(256, 8, 3, 2, 8).transpose(2, 0, 1, 3, 4).reshape(3, 256, 128)
    my, ty = 2 * (r % 96) + r // 192, (r // 96) % 2
    k = np.arange(192)
    jy = 12 * (k % 16) + k // 16
    yf = trig(my[:, None], ty[:, None], jy[None])
    yi = (yf * weight(my)[:, None]).T
    mx, tx = 64 * (r // 128) + r % 64, (r // 64) % 2
    lane = np.arange(128)
    jx = 24 * (2 * (lane[None] // 24) + np.arange(2)[:, None]) + lane[None] % 24
    xf = np.where(lane[None, :, None] < 96, trig(mx[None, None], tx[None, None], jx[:, :, None]), 0.0)
    xi = np.swapaxes(xf * weight(mx)[None, None], 1, 2)
    stack = lambda t: np.stack(pair_np(t), axis=-3)
    wide = lambda t: np.concatenate([pair_np(t)[0], pair_np(t)[0], pair_np(t)[1]], axis=-1)
    return [stack(zf), wide(yf), stack(xf), stack(xi), wide(yi), stack(zi)]


def split(x):
    hi = x.astype(bf16)
    lo = (x - hi.astype(f32)).astype(bf16)
    return hi, lo


def cat(parts, axis):
    return jnp.concatenate(parts, axis=axis)


def lanes(shape):
    return lax.broadcasted_iota(jnp.int32, shape, len(shape) - 1)


def dot(a, b, rhs_t=False):
    return lax.dot_general(a, b, (((1,), (1 if rhs_t else 0,)), ((), ())), preferred_element_type=f32)


def padded_line(vort, c, y, lane):
    a, b, d = [vort[c, :, pl.ds(384 * (y // 2) + 128 * i, 128)] for i in range(3)]
    if y % 2 == 0:
        return a, jnp.where(lane < 64, b, 0.0)
    rb, rd = pltpu.roll(b, 64, 1), pltpu.roll(d, 64, 1)
    return jnp.where(lane < 64, rb, rd), jnp.where(lane < 64, rd, 0.0)


def z_forward(vort, zf, out, w):
    lane = lanes((24, 128))
    for y in range(12):
        for c in range(3):
            v0, v1 = padded_line(vort, c, y, lane)
            r0 = y * 72 + c * 24
            w[pl.ds(r0, 24), pl.ds(0, 128)] = v0
            w[pl.ds(r0, 24), pl.ds(128, 128)] = v1
    w[pl.ds(864, 32), :] = jnp.zeros((32, 256), f32)
    table = cat([zf[0], zf[0], zf[1]], 1)
    for blk, n in ((0, 256), (256, 256), (512, 256), (768, 128)):
        hi, lo = split(w[pl.ds(blk, n), :])
        acc = dot(table, cat([hi, lo, hi], 1), rhs_t=True)
        for jj in range(n // 128):
            out[:, :, blk // 128 + jj] = acc[:, 128 * jj : 128 * jj + 128].reshape(8, 6, 8, 128)


def y_forward(g, h2, r, ty, out, s):
    zm = 2 * g + h2
    lane = lanes((8, 128))
    zero = jnp.zeros((8, 128), f32)
    for y in range(12):
        for c in range(3):
            j, o = divmod(24 * (3 * y + c), 128)
            for qh in range(2):
                v = zero
                for pp in (3, 2, 1, 0):
                    t = r[g, pp, qh, h2, j]
                    if o + 24 > 128:
                        t = jnp.where(lane >= o, t, r[g, pp, qh, h2, j + 1])
                    t = pltpu.roll(t, (24 * pp - o) % 128, 1)
                    v = jnp.where(lane < 24 * pp + 24, t, v)
                s[pl.ds(8 * (2 * y + qh), 8), pl.ds(128 * c, 128)] = v
    hi, lo = split(s[...])
    acc = dot(ty[...], cat([hi, lo, hi], 0))
    for h in range(2):
        for c in range(3):
            out[h, 3 * zm + c] = acc[192 * h : 192 * h + 192, 128 * c : 128 * c + 128]


def green_table(chip, core, out):
    unit = 2.0 * math.pi / N
    lane = lanes((8, 128))
    row = lax.broadcasted_iota(jnp.int32, (8, 128), 0)

    def body(it, _):
        kz = (3 * chip + it // 12).astype(f32) * unit
        ky = (16 * (it % 12) + core + 2 * row).astype(f32) * unit
        for tl in range(3):
            kx = (64 * tl + lane % 64).astype(f32) * unit
            sq = kx * kx + ky * ky + kz * kz
            green = jnp.exp(-0.5 * sq) / (sq + jnp.where(sq == 0.0, 1.0, 0.0))
            out[pl.ds(pl.multiple_of(8 * it, 8), 8), pl.ds(128 * tl, 128)] = green
        return 0

    lax.fori_loop(0, 36, body, 0)


B = 48


def x_stage(g, chip, core, yt, th, xf, xi, gt, ub, uo, f, u, done):
    unit = 2.0 * math.pi / N
    lane = lanes((8, 128))
    row = lax.broadcasted_iota(jnp.int32, (8, 128), 0)
    sign = jnp.where(lane < 64, 1.0, -1.0)
    kz = (3 * chip + g).astype(f32) * unit
    combos = [(t, c, s) for t in range(2) for c in range(3) for s in range(2)]
    at = lambda t, c, s: ((t * 3 + c) * 2 + s) * B
    tf = cat([xf[core, 0], xf[1 - core, 0], xf[core, 0], xf[1 - core, 0], xf[core, 1], xf[1 - core, 1]], 0)
    for ib in range(2):
        parts = []
        for t, c, s in combos:
            rows = pl.ds(96 * s + B * ib, B)
            zmc = 6 * g + 3 * t + c
            parts.append(cat([yt[core, zmc, rows, :], th[zmc, rows, :]], 1))
        hi, lo = split(cat(parts, 0))
        f[ib] = dot(cat([hi, lo, hi], 1), tf)
    for ib in range(2):
        for rt in range(B // 8):
            i0 = B * ib + 8 * rt
            ky = (2 * i0 + core + 2 * row).astype(f32) * unit
            for tl in range(3):
                kxs = (64 * tl + lane % 64).astype(f32) * unit * sign
                ls = pl.ds(128 * tl, 128)
                green = gt[pl.ds(pl.multiple_of(96 * g + i0, 8), 8), ls]
                pt = {k: f[ib, pl.ds(at(*k) + 8 * rt, 8), ls] * green for k in combos}
                for t in range(2):
                    dz = lambda c, s: (kz if t == 0 else -kz) * pt[1 - t, c, s]
                    for s in range(2):
                        dy = lambda c: (ky if s == 0 else -ky) * pt[t, c, 1 - s]
                        dx = lambda c: kxs * pltpu.roll(pt[t, c, s], 64, 1)
                        u[ib, pl.ds(at(t, 0, s) + 8 * rt, 8), ls] = dy(2) - dz(1, s)
                        u[ib, pl.ds(at(t, 1, s) + 8 * rt, 8), ls] = dz(0, s) - dx(2)
                        u[ib, pl.ds(at(t, 2, s) + 8 * rt, 8), ls] = dx(1) - dy(0)
    k0 = cat([xi[core, 0], xi[1 - core, 0]], 1)
    k1 = cat([xi[core, 1], xi[1 - core, 1]], 1)
    ti = cat([k0, k0, k1], 0)
    for ib in range(2):
        hi, lo = split(u[ib])
        back = dot(cat([hi, lo, hi], 1), ti)
        for t, c, s in combos:
            zmc = 6 * g + 3 * t + c
            r0 = at(t, c, s)
            ub[core, zmc, s, pl.ds(B * ib, B), :] = back[r0 : r0 + B, :128]
            uo[zmc, s, pl.ds(B * ib, B), :] = back[r0 : r0 + B, 128:]
        done(ib)


def y_backward(g, h2, ub, ty, out, o):
    zm = 2 * g + h2
    lane = lanes((8, 128))
    rhs = cat([cat([ub[h, 3 * zm + c, i] for c in range(3)], 1) for h in range(2) for i in range(2)], 0)
    hi, lo = split(rhs)
    o[...] = dot(ty[...], cat([hi, lo, hi], 0))
    for pp in range(4):
        for qh in range(2):
            for j in range(7):
                v = None
                for i in range((128 * j) // 24, min((128 * j + 127) // 24, 35) + 1):
                    y, c = divmod(i, 3)
                    t = o[pl.ds(8 * (2 * y + qh), 8), pl.ds(128 * c, 128)]
                    t = pltpu.roll(t, (24 * i - 128 * j - 24 * pp) % 128, 1)
                    v = t if v is None else jnp.where(lane >= 24 * i - 128 * j, t, v)
                out[g, pp, qh, h2, j] = v


def z_backward(g, v, zi, acc, flow):
    table = cat([zi[g, 0], zi[g, 0], zi[g, 1]], 1)
    for j in (0, 2, 4, 6):
        n = min(2, 7 - j)
        rhs = cat([v[:, 2 * g : 2 * g + 2, j + i].reshape(128, 128) for i in range(n)], 1)
        hi, lo = split(rhs)
        part = dot(table, cat([hi, lo, hi], 0))
        ls = pl.ds(128 * j, 128 * n)
        if g == 0:
            acc[:, ls] = part
        elif g == 1:
            acc[:, ls] = acc[:, ls] + part
        else:
            flow[ls, :] = (acc[:, ls] + part).T


def diff(m2, m1, p1, p2):
    return (8.0 * (p1 - m1) - (p2 - m2)) * (1.0 / 12.0)


def put(out, c, yp, pair):
    lane = lanes((24, 128))
    (a0, b0), (a1, b1) = [(v[:, :128], v[:, 128:]) for v in pair]
    ra, rb = pltpu.roll(a1, 64, 1), pltpu.roll(b1, 64, 1)
    out[c, :, pl.ds(384 * yp, 128)] = a0
    out[c, :, pl.ds(384 * yp + 128, 128)] = jnp.where(lane < 64, b0, ra)
    out[c, :, pl.ds(384 * yp + 256, 128)] = jnp.where(lane < 64, ra, rb)


def inner_stretch(flow, w, part):
    row = lax.broadcasted_iota(jnp.int32, (24, 256), 0)
    zero = jnp.zeros((24, 256), f32)
    for y in range(12):
        for c in range(3):
            i = 3 * y + c
            line = lambda k: flow[pl.ds(24 * (3 * k + c), 24), :] if 0 <= k < 12 else zero
            cur = line(y)
            dx = diff(*[
                jnp.where(jnp.logical_and(row + k >= 0, row + k < 24), pltpu.roll(cur, (-k) % 24, 0), zero)
                for k in (-2, -1, 1, 2)
            ])
            dy = diff(*[line(y + k) for k in (-2, -1, 1, 2)])
            dz = diff(*[pltpu.roll(cur, (-k) % 256, 1) for k in (-2, -1, 1, 2)])
            wv = [w[pl.ds(72 * y + 24 * d, 24), :] for d in range(3)]
            part[pl.ds(24 * i, 24), :] = wv[0] * dx + wv[1] * dy + wv[2] * dz


def edge_stretch(w, part, xr, yr, top, low, st):
    zero = jnp.zeros((24, 256), f32)
    for i in range(36):
        top[i, pl.ds(6, 2), :] = xr[0, i // 4, pl.ds(2 * (i % 4), 2), :]
        low[i, pl.ds(10, 2), :] = xr[1, i // 4, pl.ds(2 * (i % 4), 2), :]
    for c in range(3):
        for yp in range(6):
            pair = []
            for y in (2 * yp, 2 * yp + 1):
                i = 3 * y + c
                v = part[pl.ds(24 * i, 24), :]
                wx = w[pl.ds(72 * y, 24), :]
                head = diff(*[top[i, pl.ds(8 + k, 8), :] for k in (-2, -1, 1, 2)])
                tail = diff(*[low[i, pl.ds(2 + k, 8), :] for k in (-2, -1, 1, 2)])
                v = cat([v[0:8] + wx[0:8] * head, v[8:16], v[16:24] + wx[16:24] * tail], 0)
                if y < 2 or y > 9:
                    def line(k):
                        if k < 0:
                            return yr[0, pl.ds(((k + 2) * 3 + c) * 24, 24), :]
                        return yr[1, pl.ds(((k - 12) * 3 + c) * 24, 24), :] if k >= 12 else zero

                    dy = diff(*[line(y + k) for k in (-2, -1, 1, 2)])
                    v = v + w[pl.ds(72 * y + 24, 24), :] * dy
                pair.append(v)
            put(st, c, yp, pair)


def hops(offset):
    return sum(min(v, 4 - v) for v in offset)


OFFSETS = sorted(itertools.product((2, 1, 3, 0), repeat=3), key=hops, reverse=True)
HALF = [d for d in OFFSETS if d[2] % 2 == 0]


def flow_kernel(
    vort_h, zf_h, yf_h, xf_h, xi_h, yi_h, zi_h,
    vel, st,
    zf, yf, xf, xi, yi, zi, vort, w, zt, rv, yt, th, ub, uo, bk, vv, gt, s, o, f, u, acc, xs,
    flow, xr, yr, part, top, low,
    tsem, fs, fr, bs, br, d1, d2, hs,
):
    p, q = lax.axis_index("px"), lax.axis_index("py")
    core, half, qc = q % 2, p % 2, q // 2
    other = q + 1 - 2 * core
    mz, my, mx = p % 4, 2 * (p // 4) + q // 8, qc % 4
    chip = p * 8 + qc
    own = half == core
    loads = [
        pltpu.make_async_copy(a, b, tsem.at[i])
        for i, (a, b) in enumerate([(vort_h, vort), (zf_h, zf), (yf_h, yf), (xf_h, xf), (xi_h, xi), (yi_h, yi), (zi_h, zi)])
    ]
    for cp in loads:
        cp.start()

    near = [(p > 0, (p - 1, q)), (p < 7, (p + 1, q)), (q > 0, (p, q - 1)), (q < 15, (p, q + 1))]
    bar = pltpu.get_barrier_semaphore()

    for i in range(64):
        pl.semaphore_signal(bar, inc=1, device_id=(2 * (i // 16) + core, i % 16), device_id_type=MESH)
    pl.semaphore_signal(bar, inc=1, device_id=(p, other), device_id_type=MESH)
    for has, dev in near:
        @pl.when(has)
        def _(dev=dev):
            pl.semaphore_signal(bar, inc=1, device_id=dev, device_id_type=MESH)

    loads[0].wait()
    loads[1].wait()
    z_forward(vort, zf, zt.reshape(8, 6, 7, 8, 128), w)
    pl.semaphore_wait(bar, 65 + sum(has.astype(jnp.int32) for has, _ in near))

    def send(cond, sr, ds, ssem, rsem, dev):
        remote = pltpu.make_async_remote_copy(sr, ds, ssem, rsem, device_id=dev, device_id_type=MESH)
        if cond is None:
            remote.start()
            return

        @pl.when(cond)
        def _():
            pltpu.make_async_copy(sr, ds, rsem).start()

        @pl.when(jnp.logical_not(cond))
        def _():
            remote.start()

    def forward(g, _):
        ds = rv.at[g, p // 2, q // 8, :, :, q % 8]
        for dx, dy, dz in OFFSETS:
            x, y, z = (mx + dx) % 4, (my + dy) % 4, (mz + dz) % 4
            a, b = (y // 2) * 4 + z, (y % 2) * 4 + x
            last = own if (dx, dy, dz) == (0, 0, 0) else None
            send(last, zt.at[a, pl.ds(2 * g, 2), :, b], ds, fs, fr.at[g], (a, 2 * b + half))
        return 0

    lax.fori_loop(0, 3, forward, 0)
    green_table(chip, core, gt)
    top[...] = jnp.zeros(top.shape, f32)
    low[...] = jnp.zeros(low.shape, f32)

    rows_in = rv.reshape(3, 4, 2, 2, 7, 8, 128)
    rows_out = bk.reshape(3, 4, 2, 2, 7, 8, 128)

    def swap1(g, t):
        rows = pl.ds(6 * g + 3 * t, 3)
        return pltpu.make_async_remote_copy(
            yt.at[1 - core, rows], th.at[rows], d1.at[0, g, t], d1.at[1, g, t],
            device_id=(p, other), device_id_type=MESH,
        )

    def swap2(g, ib):
        cut = lambda ref: ref.at[pl.ds(6 * g, 6), :, pl.ds(B * ib, B), :]
        return pltpu.make_async_remote_copy(
            cut(uo), cut(ub.at[core]), d2.at[0, g, ib], d2.at[1, g, ib], device_id=(p, other), device_id_type=MESH,
        )

    def arrive(g):
        t = rv.at[g]
        pltpu.make_async_copy(t, t, fr.at[g]).wait()

        for t in range(2):
            y_forward(g, t, rows_in, yf, yt, s.at[t])
            swap1(g, t).start()

    for cp in loads[2:]:
        cp.wait()
    arrive(0)

    def group(g, _):
        swap1(g, 0).wait_recv()
        swap1(g, 1).wait_recv()
        x_stage(g, chip, core, yt, th, xf, xi, gt, ub, uo, f, u, lambda ib: swap2(g, ib).start())

        @pl.when(g < 2)
        def _():
            arrive(g + 1)

        for ib in range(2):
            swap2(g, ib).wait_recv()

        for t in range(2):
            y_backward(g, t, ub, yi, rows_out, o.at[t])

        ds = vv.at[p, pl.ds(2 * g, 2), :, qc]
        for dc in (1, 0):
            for dx, dy, dz in HALF:
                x, y, z = (mx + dx) % 4, (my + dy) % 4, (mz + dz + (half + core) % 2) % 4
                a, b = (y // 2) * 4 + z, (y % 2) * 8 + 2 * x + (core + dc) % 2
                last = own if (dx, dy, dz, dc) == (0, 0, 0, 0) else None
                send(last, bk.at[g, a // 2, b // 8, :, :, b % 8], ds, bs, br.at[g], (a, b))
        return 0

    lax.fori_loop(0, 3, group, 0)

    vin = vv.reshape(8, 6, 7, 8, 128)
    for g in range(3):
        t = vv.at[:, pl.ds(2 * g, 2)]
        pltpu.make_async_copy(t, t, br.at[g]).wait()
        z_backward(g, vin, zi, acc, flow)

    for m in range(9):
        for e, r0 in ((0, 0), (1, 22)):
            for i in range(4):
                xs[e, m, pl.ds(2 * i, 2), :] = flow[pl.ds(24 * (4 * m + i) + r0, 2), :]
    srcs = [xs.at[0], xs.at[1], flow.at[pl.ds(0, 144)], flow.at[pl.ds(720, 144)]]
    dsts = [xr.at[1], xr.at[0], yr.at[1], yr.at[0]]
    back = [1, 0, 3, 2]
    cps = []
    for k, (has, dev) in enumerate(near):
        cps.append(pltpu.make_async_remote_copy(srcs[k], dsts[k], hs.at[0, k], hs.at[1, k], device_id=dev, device_id_type=MESH))

        @pl.when(has)
        def _(k=k):
            cps[k].start()

    ends = [xr.at[0], xr.at[1], yr.at[0], yr.at[1]]
    for k, ref in enumerate(ends):
        @pl.when(jnp.logical_not(near[k][0]))
        def _(ref=ref):
            ref[...] = jnp.zeros(ref.shape, f32)

    for yp in range(6):
        for c in range(3):
            put(vel, c, yp, [flow[pl.ds(24 * (3 * (2 * yp + e) + c), 24), :] for e in range(2)])
    inner_stretch(flow, w, part)

    for g in range(3):
        swap1(g, 0).wait_send()
        swap1(g, 1).wait_send()
        for ib in range(2):
            swap2(g, ib).wait_send()
    flat = [zt.reshape(2688, 1, 128), bk.reshape(2688, 1, 128)]
    for n, cond in ((63, own), (64, jnp.logical_not(own))):
        @pl.when(cond)
        def _(n=n):
            for ref, sem in zip(flat, (fs, bs)):
                t = ref.at[pl.ds(0, 42 * n)]
                pltpu.make_async_copy(t, t, sem).wait()

    for k, (has, dev) in enumerate(near):
        @pl.when(has)
        def _(k=k):
            cps[k].wait_send()
            cps[back[k]].wait_recv()

    edge_stretch(w, part, xr, yr, top, low, st)


def sds(*shape):
    return jax.ShapeDtypeStruct(shape, f32)


def on_device(tb, vort):
    vspec, aspec = pl.BlockSpec(memory_space=VMEM), pl.BlockSpec(memory_space=ANY)
    dma = pltpu.SemaphoreType.DMA
    vel, st = pl.pallas_call(
        flow_kernel,
        out_shape=[VMEM((3, 24, 2304), f32)] * 2,
        in_specs=[aspec] * 7,
        out_specs=[vspec] * 2,
        scratch_shapes=[VMEM(t.shape, bf16) for t in tb]
        + [
            VMEM((3, 24, 2304), f32), VMEM((896, 256), f32), VMEM((8, 6, 7, 8, 1, 128), f32), VMEM((3, 4, 2, 2, 7, 8, 1, 128), f32),
            VMEM((2, 18, 192, 128), f32), VMEM((18, 192, 128), f32), VMEM((2, 18, 2, 96, 128), f32),
            VMEM((18, 2, 96, 128), f32), VMEM((3, 4, 2, 2, 7, 8, 1, 128), f32), VMEM((8, 6, 7, 8, 1, 128), f32),
            VMEM((288, 384), f32), VMEM((2, 192, 384), f32), VMEM((2, 192, 384), f32),
            VMEM((2, 576, 384), f32), VMEM((2, 576, 384), f32), VMEM((256, 896), f32), VMEM((2, 9, 8, 256), f32),
            VMEM((896, 256), f32), VMEM((2, 9, 8, 256), f32), VMEM((2, 144, 256), f32),
            VMEM((896, 256), f32),
            VMEM((36, 24, 256), f32), VMEM((36, 24, 256), f32),
            dma((7,)), dma, dma((3,)), dma, dma((3,)), dma((2, 3, 2)), dma((2, 3, 2)), dma((2, 4)),
        ],
        compiler_params=pltpu.CompilerParams(collective_id=0, has_side_effects=True, vmem_limit_bytes=58 * 1024 * 1024),
    )(vort, *tb)
    return pl.pallas_call(
        hand_over,
        out_shape=[sds(3, 24, 2304)] * 2,
        in_specs=[vspec] * 2,
        out_specs=[aspec] * 2,
        scratch_shapes=[dma((2, 3))],
        compiler_params=pltpu.CompilerParams(vmem_limit_bytes=30 * 1024 * 1024),
    )(vel, st)


def hand_over(vel, st, vel_o, st_o, sem):
    outs = [pltpu.make_async_copy(x.at[c], o.at[c], sem.at[k, c]) for k, (x, o) in enumerate(((vel, vel_o), (st, st_o))) for c in range(3)]
    for cp in outs:
        cp.start()
    for cp in outs:
        cp.wait()


def solution(mesh):
    tb = [jnp.asarray(v) for v in tables()]
    return jax.shard_map(
        functools.partial(on_device, tb), mesh=mesh, in_specs=(P(None, "px", "py"),),
        out_specs=(P(None, "px", "py"), P(None, "px", "py")), check_vma=False,
    )
```

```python
import math
import functools
import itertools

import numpy as np
import jax
import jax.numpy as jnp
from jax import lax
from jax.experimental import pallas as pl
from jax.experimental.pallas import tpu as pltpu
from jax.sharding import PartitionSpec as P

G = 192
N = 2 * G
MESH = pl.DeviceIdType.MESH
VMEM = pltpu.VMEM
ANY = pl.ANY
bf16 = jnp.bfloat16
f32 = jnp.float32


def pair_np(t):
    hi = np.asarray(t, np.float32).astype(jnp.bfloat16)
    lo = (t - hi.astype(np.float64)).astype(np.float32).astype(jnp.bfloat16)
    return hi, lo


def trig(m, t, j):
    a = 2.0 * np.pi * ((m * j) % N) / N
    return np.where(t == 0, np.cos(a), np.sin(a))


def weight(m):
    return np.where(m == 0, 1.0, 2.0) / N


def tables():
    r = np.arange(384)
    dg, zm, dl = r // 48, (r // 8) % 6, r % 8
    mz, tz = 3 * (8 * dg + dl) + zm // 2, zm % 2
    z = np.arange(256)
    zf = np.where(z[None] < G, trig(mz[:, None], tz[:, None], z[None]), 0.0)
    zi = (zf * weight(mz)[:, None]).T.reshape(256, 8, 3, 2, 8).transpose(2, 0, 1, 3, 4).reshape(3, 256, 128)
    my, ty = 2 * (r % 96) + r // 192, (r // 96) % 2
    k = np.arange(192)
    jy = 12 * (k % 16) + k // 16
    yf = trig(my[:, None], ty[:, None], jy[None])
    yi = (yf * weight(my)[:, None]).T
    mx, tx = 64 * (r // 128) + r % 64, (r // 64) % 2
    lane = np.arange(128)
    jx = 24 * (2 * (lane[None] // 24) + np.arange(2)[:, None]) + lane[None] % 24
    xf = np.where(lane[None, :, None] < 96, trig(mx[None, None], tx[None, None], jx[:, :, None]), 0.0)
    xi = np.swapaxes(xf * weight(mx)[None, None], 1, 2)
    stack = lambda t: np.stack(pair_np(t), axis=-3)
    wide = lambda t: np.concatenate([pair_np(t)[0], pair_np(t)[0], pair_np(t)[1]], axis=-1)
    return [stack(zf), wide(yf), stack(xf), stack(xi), wide(yi), stack(zi)]


def split(x):
    hi = x.astype(bf16)
    lo = (x - hi.astype(f32)).astype(bf16)
    return hi, lo


def cat(parts, axis):
    return jnp.concatenate(parts, axis=axis)


def lanes(shape):
    return lax.broadcasted_iota(jnp.int32, shape, len(shape) - 1)


def dot(a, b, rhs_t=False):
    return lax.dot_general(a, b, (((1,), (1 if rhs_t else 0,)), ((), ())), preferred_element_type=f32)


def padded_line(vort, c, y, lane):
    a, b, d = [vort[c, :, pl.ds(384 * (y // 2) + 128 * i, 128)] for i in range(3)]
    if y % 2 == 0:
        return a, jnp.where(lane < 64, b, 0.0)
    rb, rd = pltpu.roll(b, 64, 1), pltpu.roll(d, 64, 1)
    return jnp.where(lane < 64, rb, rd), jnp.where(lane < 64, rd, 0.0)


def z_forward(vort, zf, out, w):
    lane = lanes((24, 128))
    for y in range(12):
        for c in range(3):
            v0, v1 = padded_line(vort, c, y, lane)
            r0 = y * 72 + c * 24
            w[pl.ds(r0, 24), pl.ds(0, 128)] = v0
            w[pl.ds(r0, 24), pl.ds(128, 128)] = v1
    w[pl.ds(864, 32), :] = jnp.zeros((32, 256), f32)
    table = cat([zf[0], zf[0], zf[1]], 1)
    for blk, n in ((0, 256), (256, 256), (512, 256), (768, 128)):
        hi, lo = split(w[pl.ds(blk, n), :])
        acc = dot(table, cat([hi, lo, hi], 1), rhs_t=True)
        for jj in range(n // 128):
            out[:, :, blk // 128 + jj] = acc[:, 128 * jj : 128 * jj + 128].reshape(8, 6, 8, 128)


def y_forward(g, h2, r, ty, out, s):
    zm = 2 * g + h2
    lane = lanes((8, 128))
    zero = jnp.zeros((8, 128), f32)
    for y in range(12):
        for c in range(3):
            j, o = divmod(24 * (3 * y + c), 128)
            for qh in range(2):
                v = zero
                for pp in (3, 2, 1, 0):
                    t = r[g, pp, qh, h2, j]
                    if o + 24 > 128:
                        t = jnp.where(lane >= o, t, r[g, pp, qh, h2, j + 1])
                    t = pltpu.roll(t, (24 * pp - o) % 128, 1)
                    v = jnp.where(lane < 24 * pp + 24, t, v)
                s[pl.ds(8 * (2 * y + qh), 8), pl.ds(128 * c, 128)] = v
    hi, lo = split(s[...])
    acc = dot(ty[...], cat([hi, lo, hi], 0))
    for h in range(2):
        for c in range(3):
            out[h, 3 * zm + c] = acc[192 * h : 192 * h + 192, 128 * c : 128 * c + 128]


def green_table(chip, core, out):
    unit = 2.0 * math.pi / N
    lane = lanes((8, 128))
    row = lax.broadcasted_iota(jnp.int32, (8, 128), 0)

    def body(it, _):
        kz = (3 * chip + it // 12).astype(f32) * unit
        ky = (16 * (it % 12) + core + 2 * row).astype(f32) * unit
        for tl in range(3):
            kx = (64 * tl + lane % 64).astype(f32) * unit
            sq = kx * kx + ky * ky + kz * kz
            green = jnp.exp(-0.5 * sq) / (sq + jnp.where(sq == 0.0, 1.0, 0.0))
            out[pl.ds(pl.multiple_of(8 * it, 8), 8), pl.ds(128 * tl, 128)] = green
        return 0

    lax.fori_loop(0, 36, body, 0)


B = 48


def x_stage(g, chip, core, yt, th, xf, xi, gt, ub, uo, f, u, done):
    unit = 2.0 * math.pi / N
    lane = lanes((8, 128))
    row = lax.broadcasted_iota(jnp.int32, (8, 128), 0)
    sign = jnp.where(lane < 64, 1.0, -1.0)
    kz = (3 * chip + g).astype(f32) * unit
    combos = [(t, c, s) for t in range(2) for c in range(3) for s in range(2)]
    at = lambda t, c, s: ((t * 3 + c) * 2 + s) * B
    tf = cat([xf[core, 0], xf[1 - core, 0], xf[core, 0], xf[1 - core, 0], xf[core, 1], xf[1 - core, 1]], 0)
    for ib in range(2):
        parts = []
        for t, c, s in combos:
            rows = pl.ds(96 * s + B * ib, B)
            zmc = 6 * g + 3 * t + c
            parts.append(cat([yt[core, zmc, rows, :], th[zmc, rows, :]], 1))
        hi, lo = split(cat(parts, 0))
        f[ib] = dot(cat([hi, lo, hi], 1), tf)
    for ib in range(2):
        for rt in range(B // 8):
            i0 = B * ib + 8 * rt
            ky = (2 * i0 + core + 2 * row).astype(f32) * unit
            for tl in range(3):
                kxs = (64 * tl + lane % 64).astype(f32) * unit * sign
                ls = pl.ds(128 * tl, 128)
                green = gt[pl.ds(pl.multiple_of(96 * g + i0, 8), 8), ls]
                pt = {k: f[ib, pl.ds(at(*k) + 8 * rt, 8), ls] * green for k in combos}
                for t in range(2):
                    dz = lambda c, s: (kz if t == 0 else -kz) * pt[1 - t, c, s]
                    for s in range(2):
                        dy = lambda c: (ky if s == 0 else -ky) * pt[t, c, 1 - s]
                        dx = lambda c: kxs * pltpu.roll(pt[t, c, s], 64, 1)
                        u[ib, pl.ds(at(t, 0, s) + 8 * rt, 8), ls] = dy(2) - dz(1, s)
                        u[ib, pl.ds(at(t, 1, s) + 8 * rt, 8), ls] = dz(0, s) - dx(2)
                        u[ib, pl.ds(at(t, 2, s) + 8 * rt, 8), ls] = dx(1) - dy(0)
    k0 = cat([xi[core, 0], xi[1 - core, 0]], 1)
    k1 = cat([xi[core, 1], xi[1 - core, 1]], 1)
    ti = cat([k0, k0, k1], 0)
    for ib in range(2):
        hi, lo = split(u[ib])
        back = dot(cat([hi, lo, hi], 1), ti)
        for t, c, s in combos:
            zmc = 6 * g + 3 * t + c
            r0 = at(t, c, s)
            ub[core, zmc, s, pl.ds(B * ib, B), :] = back[r0 : r0 + B, :128]
            uo[zmc, s, pl.ds(B * ib, B), :] = back[r0 : r0 + B, 128:]
        done(ib)


def y_backward(g, h2, ub, ty, out, o):
    zm = 2 * g + h2
    lane = lanes((8, 128))
    rhs = cat([cat([ub[h, 3 * zm + c, i] for c in range(3)], 1) for h in range(2) for i in range(2)], 0)
    hi, lo = split(rhs)
    o[...] = dot(ty[...], cat([hi, lo, hi], 0))
    for pp in range(4):
        for qh in range(2):
            for j in range(7):
                v = None
                for i in range((128 * j) // 24, min((128 * j + 127) // 24, 35) + 1):
                    y, c = divmod(i, 3)
                    t = o[pl.ds(8 * (2 * y + qh), 8), pl.ds(128 * c, 128)]
                    t = pltpu.roll(t, (24 * i - 128 * j - 24 * pp) % 128, 1)
                    v = t if v is None else jnp.where(lane >= 24 * i - 128 * j, t, v)
                out[g, pp, qh, h2, j] = v


def z_backward(g, v, zi, acc, flow):
    table = cat([zi[g, 0], zi[g, 0], zi[g, 1]], 1)
    for j in (0, 2, 4, 6):
        n = min(2, 7 - j)
        rhs = cat([v[:, 2 * g : 2 * g + 2, j + i].reshape(128, 128) for i in range(n)], 1)
        hi, lo = split(rhs)
        part = dot(table, cat([hi, lo, hi], 0))
        ls = pl.ds(128 * j, 128 * n)
        if g == 0:
            acc[:, ls] = part
        elif g == 1:
            acc[:, ls] = acc[:, ls] + part
        else:
            flow[ls, :] = (acc[:, ls] + part).T


def diff(m2, m1, p1, p2):
    return (8.0 * (p1 - m1) - (p2 - m2)) * (1.0 / 12.0)


def put(out, c, yp, pair):
    lane = lanes((24, 128))
    (a0, b0), (a1, b1) = [(v[:, :128], v[:, 128:]) for v in pair]
    ra, rb = pltpu.roll(a1, 64, 1), pltpu.roll(b1, 64, 1)
    out[c, :, pl.ds(384 * yp, 128)] = a0
    out[c, :, pl.ds(384 * yp + 128, 128)] = jnp.where(lane < 64, b0, ra)
    out[c, :, pl.ds(384 * yp + 256, 128)] = jnp.where(lane < 64, ra, rb)


def inner_stretch(flow, w, part):
    row = lax.broadcasted_iota(jnp.int32, (24, 256), 0)
    zero = jnp.zeros((24, 256), f32)
    for y in range(12):
        for c in range(3):
            i = 3 * y + c
            line = lambda k: flow[pl.ds(24 * (3 * k + c), 24), :] if 0 <= k < 12 else zero
            cur = line(y)
            dx = diff(*[
                jnp.where(jnp.logical_and(row + k >= 0, row + k < 24), pltpu.roll(cur, (-k) % 24, 0), zero)
                for k in (-2, -1, 1, 2)
            ])
            dy = diff(*[line(y + k) for k in (-2, -1, 1, 2)])
            dz = diff(*[pltpu.roll(cur, (-k) % 256, 1) for k in (-2, -1, 1, 2)])
            wv = [w[pl.ds(72 * y + 24 * d, 24), :] for d in range(3)]
            part[pl.ds(24 * i, 24), :] = wv[0] * dx + wv[1] * dy + wv[2] * dz


def edge_stretch(w, part, xr, yr, top, low, st):
    zero = jnp.zeros((24, 256), f32)
    for i in range(36):
        top[i, pl.ds(6, 2), :] = xr[0, i // 4, pl.ds(2 * (i % 4), 2), :]
        low[i, pl.ds(10, 2), :] = xr[1, i // 4, pl.ds(2 * (i % 4), 2), :]
    for c in range(3):
        for yp in range(6):
            pair = []
            for y in (2 * yp, 2 * yp + 1):
                i = 3 * y + c
                v = part[pl.ds(24 * i, 24), :]
                wx = w[pl.ds(72 * y, 24), :]
                head = diff(*[top[i, pl.ds(8 + k, 8), :] for k in (-2, -1, 1, 2)])
                tail = diff(*[low[i, pl.ds(2 + k, 8), :] for k in (-2, -1, 1, 2)])
                v = cat([v[0:8] + wx[0:8] * head, v[8:16], v[16:24] + wx[16:24] * tail], 0)
                if y < 2 or y > 9:
                    def line(k):
                        if k < 0:
                            return yr[0, pl.ds(((k + 2) * 3 + c) * 24, 24), :]
                        return yr[1, pl.ds(((k - 12) * 3 + c) * 24, 24), :] if k >= 12 else zero

                    dy = diff(*[line(y + k) for k in (-2, -1, 1, 2)])
                    v = v + w[pl.ds(72 * y + 24, 24), :] * dy
                pair.append(v)
            put(st, c, yp, pair)


def hops(offset):
    return sum(min(v, 4 - v) for v in offset)


OFFSETS = sorted(itertools.product((2, 1, 3, 0), repeat=3), key=hops, reverse=True)
HALF = [d for d in OFFSETS if d[2] % 2 == 0]


def flow_kernel(
    vort_h, zf_h, yf_h, xf_h, xi_h, yi_h, zi_h,
    vel, st,
    zf, yf, xf, xi, yi, zi, vort, w, zt, rv, yt, th, ub, uo, bk, vv, gt, s, o, f, u, acc, xs,
    flow, xr, yr, part, top, low,
    tsem, fs, fr, bs, br, d1, d2, hs,
):
    p, q = lax.axis_index("px"), lax.axis_index("py")
    core, half, qc = q % 2, p % 2, q // 2
    other = q + 1 - 2 * core
    mz, my, mx = p % 4, 2 * (p // 4) + q // 8, qc % 4
    chip = p * 8 + qc
    own = half == core
    loads = [
        pltpu.make_async_copy(a, b, tsem.at[i])
        for i, (a, b) in enumerate([(vort_h, vort), (zf_h, zf), (yf_h, yf), (xf_h, xf), (xi_h, xi), (yi_h, yi), (zi_h, zi)])
    ]
    for cp in loads:
        cp.start()

    near = [(p > 0, (p - 1, q)), (p < 7, (p + 1, q)), (q > 0, (p, q - 1)), (q < 15, (p, q + 1))]
    bar = pltpu.get_barrier_semaphore()

    for i in range(64):
        pl.semaphore_signal(bar, inc=1, device_id=(2 * (i // 16) + core, i % 16), device_id_type=MESH)
    pl.semaphore_signal(bar, inc=1, device_id=(p, other), device_id_type=MESH)
    for has, dev in near:
        @pl.when(has)
        def _(dev=dev):
            pl.semaphore_signal(bar, inc=1, device_id=dev, device_id_type=MESH)

    loads[0].wait()
    loads[1].wait()
    z_forward(vort, zf, zt.reshape(8, 6, 7, 8, 128), w)
    pl.semaphore_wait(bar, 65 + sum(has.astype(jnp.int32) for has, _ in near))

    def send(cond, sr, ds, ssem, rsem, dev):
        remote = pltpu.make_async_remote_copy(sr, ds, ssem, rsem, device_id=dev, device_id_type=MESH)
        if cond is None:
            remote.start()
            return

        @pl.when(cond)
        def _():
            pltpu.make_async_copy(sr, ds, rsem).start()

        @pl.when(jnp.logical_not(cond))
        def _():
            remote.start()

    def forward(g, _):
        ds = rv.at[g, p // 2, q // 8, :, :, q % 8]
        for dx, dy, dz in OFFSETS:
            x, y, z = (mx + dx) % 4, (my + dy) % 4, (mz + dz) % 4
            a, b = (y // 2) * 4 + z, (y % 2) * 4 + x
            last = own if (dx, dy, dz) == (0, 0, 0) else None
            send(last, zt.at[a, pl.ds(2 * g, 2), :, b], ds, fs, fr.at[g], (a, 2 * b + half))
        return 0

    lax.fori_loop(0, 3, forward, 0)
    green_table(chip, core, gt)
    top[...] = jnp.zeros(top.shape, f32)
    low[...] = jnp.zeros(low.shape, f32)

    rows_in = rv.reshape(3, 4, 2, 2, 7, 8, 128)
    rows_out = bk.reshape(3, 4, 2, 2, 7, 8, 128)

    def swap1(g, t):
        rows = pl.ds(6 * g + 3 * t, 3)
        return pltpu.make_async_remote_copy(
            yt.at[1 - core, rows], th.at[rows], d1.at[0, g, t], d1.at[1, g, t],
            device_id=(p, other), device_id_type=MESH,
        )

    def swap2(g, ib):
        cut = lambda ref: ref.at[pl.ds(6 * g, 6), :, pl.ds(B * ib, B), :]
        return pltpu.make_async_remote_copy(
            cut(uo), cut(ub.at[core]), d2.at[0, g, ib], d2.at[1, g, ib], device_id=(p, other), device_id_type=MESH,
        )

    def arrive(g):
        t = rv.at[g]
        pltpu.make_async_copy(t, t, fr.at[g]).wait()

        for t in range(2):
            y_forward(g, t, rows_in, yf, yt, s.at[t])
            swap1(g, t).start()

    for cp in loads[2:]:
        cp.wait()
    arrive(0)

    def group(g, _):
        swap1(g, 0).wait_recv()
        swap1(g, 1).wait_recv()
        x_stage(g, chip, core, yt, th, xf, xi, gt, ub, uo, f, u, lambda ib: swap2(g, ib).start())

        @pl.when(g < 2)
        def _():
            arrive(g + 1)

        for ib in range(2):
            swap2(g, ib).wait_recv()

        for t in range(2):
            y_backward(g, t, ub, yi, rows_out, o.at[t])

        ds = vv.at[p, pl.ds(2 * g, 2), :, qc]
        for dc in (1, 0):
            for dx, dy, dz in HALF:
                x, y, z = (mx + dx) % 4, (my + dy) % 4, (mz + dz + (half + core) % 2) % 4
                a, b = (y // 2) * 4 + z, (y % 2) * 8 + 2 * x + (core + dc) % 2
                last = own if (dx, dy, dz, dc) == (0, 0, 0, 0) else None
                send(last, bk.at[g, a // 2, b // 8, :, :, b % 8], ds, bs, br.at[g], (a, b))
        return 0

    lax.fori_loop(0, 3, group, 0)

    vin = vv.reshape(8, 6, 7, 8, 128)
    for g in range(3):
        t = vv.at[:, pl.ds(2 * g, 2)]
        pltpu.make_async_copy(t, t, br.at[g]).wait()
        z_backward(g, vin, zi, acc, flow)

    srcs = [xs.at[0], xs.at[1], flow.at[pl.ds(0, 144)], flow.at[pl.ds(720, 144)]]
    dsts = [xr.at[1], xr.at[0], yr.at[1], yr.at[0]]
    back = [1, 0, 3, 2]
    cps = []
    for k, (has, dev) in enumerate(near):
        cps.append(pltpu.make_async_remote_copy(srcs[k], dsts[k], hs.at[0, k], hs.at[1, k], device_id=dev, device_id_type=MESH))

    def start(k):
        @pl.when(near[k][0])
        def _():
            cps[k].start()

    start(2)
    start(3)
    for m in range(9):
        for e, r0 in ((0, 0), (1, 22)):
            for i in range(4):
                xs[e, m, pl.ds(2 * i, 2), :] = flow[pl.ds(24 * (4 * m + i) + r0, 2), :]
    start(0)
    start(1)

    ends = [xr.at[0], xr.at[1], yr.at[0], yr.at[1]]
    for k, ref in enumerate(ends):
        @pl.when(jnp.logical_not(near[k][0]))
        def _(ref=ref):
            ref[...] = jnp.zeros(ref.shape, f32)

    for yp in range(6):
        for c in range(3):
            put(vel, c, yp, [flow[pl.ds(24 * (3 * (2 * yp + e) + c), 24), :] for e in range(2)])
    inner_stretch(flow, w, part)

    for g in range(3):
        swap1(g, 0).wait_send()
        swap1(g, 1).wait_send()
        for ib in range(2):
            swap2(g, ib).wait_send()
    flat = [zt.reshape(2688, 1, 128), bk.reshape(2688, 1, 128)]
    for n, cond in ((63, own), (64, jnp.logical_not(own))):
        @pl.when(cond)
        def _(n=n):
            for ref, sem in zip(flat, (fs, bs)):
                t = ref.at[pl.ds(0, 42 * n)]
                pltpu.make_async_copy(t, t, sem).wait()

    for k, (has, dev) in enumerate(near):
        @pl.when(has)
        def _(k=k):
            cps[k].wait_send()
            cps[back[k]].wait_recv()

    edge_stretch(w, part, xr, yr, top, low, st)


def sds(*shape):
    return jax.ShapeDtypeStruct(shape, f32)


def on_device(tb, vort):
    vspec, aspec = pl.BlockSpec(memory_space=VMEM), pl.BlockSpec(memory_space=ANY)
    dma = pltpu.SemaphoreType.DMA
    vel, st = pl.pallas_call(
        flow_kernel,
        out_shape=[VMEM((3, 24, 2304), f32)] * 2,
        in_specs=[aspec] * 7,
        out_specs=[vspec] * 2,
        scratch_shapes=[VMEM(t.shape, bf16) for t in tb]
        + [
            VMEM((3, 24, 2304), f32), VMEM((896, 256), f32), VMEM((8, 6, 7, 8, 1, 128), f32), VMEM((3, 4, 2, 2, 7, 8, 1, 128), f32),
            VMEM((2, 18, 192, 128), f32), VMEM((18, 192, 128), f32), VMEM((2, 18, 2, 96, 128), f32),
            VMEM((18, 2, 96, 128), f32), VMEM((3, 4, 2, 2, 7, 8, 1, 128), f32), VMEM((8, 6, 7, 8, 1, 128), f32),
            VMEM((288, 384), f32), VMEM((2, 192, 384), f32), VMEM((2, 192, 384), f32),
            VMEM((2, 576, 384), f32), VMEM((2, 576, 384), f32), VMEM((256, 896), f32), VMEM((2, 9, 8, 256), f32),
            VMEM((896, 256), f32), VMEM((2, 9, 8, 256), f32), VMEM((2, 144, 256), f32),
            VMEM((896, 256), f32),
            VMEM((36, 24, 256), f32), VMEM((36, 24, 256), f32),
            dma((7,)), dma, dma((3,)), dma, dma((3,)), dma((2, 3, 2)), dma((2, 3, 2)), dma((2, 4)),
        ],
        compiler_params=pltpu.CompilerParams(collective_id=0, has_side_effects=True, vmem_limit_bytes=58 * 1024 * 1024),
    )(vort, *tb)
    return pl.pallas_call(
        hand_over,
        out_shape=[sds(3, 24, 2304)] * 2,
        in_specs=[vspec] * 2,
        out_specs=[aspec] * 2,
        scratch_shapes=[dma((2, 3))],
        compiler_params=pltpu.CompilerParams(vmem_limit_bytes=30 * 1024 * 1024),
    )(vel, st)


def hand_over(vel, st, vel_o, st_o, sem):
    outs = [pltpu.make_async_copy(x.at[c], o.at[c], sem.at[k, c]) for k, (x, o) in enumerate(((vel, vel_o), (st, st_o))) for c in range(3)]
    for cp in outs:
        cp.start()
    for cp in outs:
        cp.wait()


def solution(mesh):
    tb = [jnp.asarray(v) for v in tables()]
    return jax.shard_map(
        functools.partial(on_device, tb), mesh=mesh, in_specs=(P(None, "px", "py"),),
        out_specs=(P(None, "px", "py"), P(None, "px", "py")), check_vma=False,
    )
```
